8 devices in a mesh: dp: 4 (over z, y, x), cp: 2 (over core).
Axes of the slice: x: 2, y: 2, z: 1, core: 2. Of those that a mesh axis runs over, the one named last changes fastest.
Arguments:
- inputs: bfloat16 [64, 2048, 261], P('dp', 'cp')
- latents: float32 [512, 1024], replicated
- x_gain: float32 [261], replicated
- x_shift: float32 [261], replicated
- z_gain: float32 [1024], replicated
- z_shift: float32 [1024], replicated
- w_query: bfloat16 [1024, 1024], replicated
- w_key: bfloat16 [261, 1024], replicated
- w_value: bfloat16 [261, 1024], replicated
- w_out: bfloat16 [1024, 1024], replicated
- m_gain: float32 [1024], replicated
- m_shift: float32 [1024], replicated
- w_up: bfloat16 [1024, 1024], replicated
- b_up: float32 [1024], replicated
- w_down: bfloat16 [1024, 1024], replicated
- b_down: float32 [1024], replicated
- d_out: bfloat16 [64, 512, 1024], P('dp')
Outputs:
- output 1: float32 [64, 512, 1024], P('dp')
- output 2: bfloat16 [64, 2048, 261], P('dp', 'cp')
- output 3: float32 [512, 1024], replicated
- output 4: float32 [261], replicated
- output 5: float32 [261], replicated
- output 6: float32 [1024], replicated
- output 7: float32 [1024], replicated
- output 8: float32 [1024, 1024], replicated
- output 9: float32 [261, 1024], replicated
- output 10: float32 [261, 1024], replicated
- output 11: float32 [1024, 1024], replicated
- output 12: float32 [1024], replicated
- output 13: float32 [1024], replicated
- output 14: float32 [1024, 1024], replicated
- output 15: float32 [1024], replicated
- output 16: float32 [1024, 1024], replicated
- output 17: float32 [1024], replicated
All inputs are finite; a program needn't handle non-finite values.
Results may differ from the reference program's by a relative error of at most 0.0171243.
Values sent between devices are 32-bit elements.
A program may use at most 1 GiB of HBM per device.

```python
import math
import jax
import jax.numpy as jnp
from jax import lax

BATCH = 64
INPUTS = 2048
IN_CH = 261
LATENTS = 512
WIDTH = 1024
QK_CH = 1024
V_CH = 1024
LN_EPS = 1e-5


def layer_norm(tensor, ln_gain, ln_shift):
    row_mean = jnp.mean(tensor, axis=-1, keepdims=True)
    centred = tensor - row_mean
    variance = jnp.mean(centred * centred, axis=-1, keepdims=True)
    return centred * lax.rsqrt(variance + LN_EPS) * ln_gain + ln_shift


def lowered(tensor):
    return tensor.astype(jnp.bfloat16).astype(jnp.float32)


def setup_inputs(seed: int = 0) -> dict:
    rng_keys = jax.random.split(jax.random.key(seed), 17)
    spread = 0.85 * math.sqrt(math.log(INPUTS / 16.0))

    def normal(key_index, dims_of, factor):
        return jax.random.normal(rng_keys[key_index], dims_of, jnp.float32) * factor

    return {
        'inputs': normal(0, (BATCH, INPUTS, IN_CH), 1.0).astype(jnp.bfloat16),
        'latents': normal(1, (LATENTS, WIDTH), 0.5),
        'x_gain': 1.0 + normal(2, (IN_CH,), 0.3),
        'x_shift': normal(3, (IN_CH,), 0.3),
        'z_gain': spread * (1.0 + normal(4, (WIDTH,), 0.2)),
        'z_shift': normal(5, (WIDTH,), 0.3 * spread),
        'w_query': normal(6, (WIDTH, QK_CH), WIDTH ** -0.5).astype(jnp.bfloat16),
        'w_key': normal(7, (IN_CH, QK_CH), IN_CH ** -0.5).astype(jnp.bfloat16),
        'w_value': normal(8, (IN_CH, V_CH), IN_CH ** -0.5).astype(jnp.bfloat16),
        'w_out': normal(9, (V_CH, WIDTH), 2.0 * V_CH ** -0.5).astype(jnp.bfloat16),
        'm_gain': 1.0 + normal(10, (WIDTH,), 0.2),
        'm_shift': normal(11, (WIDTH,), 0.2),
        'w_up': normal(12, (WIDTH, WIDTH), WIDTH ** -0.5).astype(jnp.bfloat16),
        'b_up': normal(13, (WIDTH,), 0.3),
        'w_down': normal(14, (WIDTH, WIDTH), WIDTH ** -0.5).astype(jnp.bfloat16),
        'b_down': normal(15, (WIDTH,), 0.3),
        'd_out': normal(16, (BATCH, LATENTS, WIDTH), 1.0).astype(jnp.bfloat16),
    }


def forward(inputs, latents, x_gain, x_shift, z_gain, z_shift, w_query, w_key, w_value, w_out, m_gain, m_shift, w_up, b_up, w_down, b_down):
    qk_scale = QK_CH ** -0.5
    z_norm = lowered(layer_norm(latents, z_gain, z_shift))
    queries = lowered(jnp.dot(z_norm, w_query, preferred_element_type=jnp.float32))

    def attend(x_rows):
        x_norm = lowered(layer_norm(x_rows.astype(jnp.float32), x_gain, x_shift))
        key_rows = lowered(jnp.dot(x_norm, w_key, preferred_element_type=jnp.float32))
        value_rows = lowered(jnp.dot(x_norm, w_value, preferred_element_type=jnp.float32))
        logits = jnp.dot(queries, key_rows.T, preferred_element_type=jnp.float32) * qk_scale
        attn_probs = lowered(jax.nn.softmax(logits, axis=-1))
        return lowered(jnp.dot(attn_probs, value_rows, preferred_element_type=jnp.float32))

    attn_out = lax.map(jax.checkpoint(attend), inputs)
    z_mid = latents + jnp.einsum('bnv,vd->bnd', attn_out, w_out)
    hidden = lowered(layer_norm(z_mid, m_gain, m_shift))
    pre_act = jnp.einsum('bnd,de->bne', hidden, w_up) + b_up
    act_val = lowered(jax.nn.gelu(pre_act))
    return z_mid + jnp.einsum('bne,ed->bnd', act_val, w_down) + b_down


def reference(inputs, latents, x_gain, x_shift, z_gain, z_shift, w_query, w_key, w_value, w_out, m_gain, m_shift, w_up, b_up, w_down, b_down, d_out):
    out_latents, pullback = jax.vjp(
        forward, inputs, latents, x_gain, x_shift, z_gain, z_shift,
        w_query.astype(jnp.float32), w_key.astype(jnp.float32), w_value.astype(jnp.float32), w_out.astype(jnp.float32),
        m_gain, m_shift, w_up.astype(jnp.float32), b_up, w_down.astype(jnp.float32), b_down)
    (d_inputs, d_latents, d_x_gain, d_x_shift, d_z_gain, d_z_shift, d_w_query, d_w_key, d_w_value, d_w_out,
     d_m_gain, d_m_shift, d_w_up, d_b_up, d_w_down, d_b_down) = pullback(d_out.astype(jnp.float32))
    return (out_latents, d_inputs, d_latents, d_x_gain, d_x_shift, d_z_gain, d_z_shift, d_w_query, d_w_key, d_w_value, d_w_out,
            d_m_gain, d_m_shift, d_w_up, d_b_up, d_w_down, d_b_down)
```

```python
import functools
import math

import jax
import jax.numpy as jnp
from jax import lax
from jax.experimental import pallas as pl
from jax.experimental.pallas import tpu as pltpu
from jax.sharding import PartitionSpec as P


LN_EPS = 1e-5
F32 = jnp.float32
BF16 = jnp.bfloat16
CH = 261
CPAD = 272
AXW = 384
ROW_GAP = 8
ACC_ROWS = 896
VEC_ROW = 784
SUM_LANE = 261
MAX_LANE = 262
INV_LANE = 263
LOG2E = math.log2(math.e)
GELU_A = math.sqrt(2.0 / math.pi)
GELU_B = 0.044715
VMEM_LIMIT = 60 * 1024 * 1024


def layer_norm(tensor, ln_gain, ln_shift):
    row_mean = jnp.mean(tensor, axis=-1, keepdims=True)
    centred = tensor - row_mean
    variance = jnp.mean(centred * centred, axis=-1, keepdims=True)
    return centred * lax.rsqrt(variance + LN_EPS) * ln_gain + ln_shift


def mm(lhs, rhs):
    return lax.dot_general(lhs, rhs, (((1,), (0,)), ((), ())), preferred_element_type=F32)


def mm_nt(lhs, rhs):
    return lax.dot_general(lhs, rhs, (((1,), (1,)), ((), ())), preferred_element_type=F32)


def mm_tn(lhs, rhs):
    return lax.dot_general(lhs, rhs, (((0,), (0,)), ((), ())), preferred_element_type=F32)


def params(semantics=1):
    return pltpu.CompilerParams(
        vmem_limit_bytes=VMEM_LIMIT, dimension_semantics=("arbitrary",) * semantics)


def cost(flops, nbytes):
    return pl.CostEstimate(flops=int(flops), bytes_accessed=int(nbytes), transcendentals=0)


def x_prep_kernel(gain_ref, shift_ref, x_ref, xn_ref, mean_ref, rstd_ref, rows_ref):
    nb = x_ref.shape[1]
    lanes = x_ref.shape[2]
    pitch = nb + ROW_GAP
    zero = jnp.zeros((nb, lanes), F32)

    def add_up(c, acc):
        return acc + x_ref[c].astype(F32)

    mean = lax.fori_loop(0, CH, add_up, zero, unroll=9) * (1.0 / CH)

    def add_sq(c, acc):
        d = x_ref[c].astype(F32) - mean
        return acc + d * d

    var = lax.fori_loop(0, CH, add_sq, zero, unroll=9) * (1.0 / CH)
    rstd = lax.rsqrt(var + LN_EPS)
    mean_ref[...] = mean
    rstd_ref[...] = rstd

    def put(c, carry):
        xn = (x_ref[c].astype(F32) - mean) * rstd * gain_ref[c] + shift_ref[c]
        rows_ref[pl.ds(pl.multiple_of(c * pitch, ROW_GAP), nb), :] = xn
        return carry

    lax.fori_loop(0, CH, put, 0, unroll=9)
    rows_ref[CH * pitch:CPAD * pitch, :] = jnp.zeros(((CPAD - CH) * pitch, lanes), F32)
    for b in range(nb):
        xn_ref[b] = rows_ref[pl.ds(b, CPAD, stride=pitch), :].astype(BF16)


def x_prep(x_cm, x_gain, x_shift):
    _, nb, m = x_cm.shape
    lanes = 128
    stat = pl.BlockSpec((nb, lanes), lambda i: (0, i))
    return pl.pallas_call(
        x_prep_kernel,
        grid=(m // lanes,),
        in_specs=[
            pl.BlockSpec(memory_space=pltpu.SMEM),
            pl.BlockSpec(memory_space=pltpu.SMEM),
            pl.BlockSpec((CH, nb, lanes), lambda i: (0, 0, i)),
        ],
        out_specs=[pl.BlockSpec((nb, CPAD, lanes), lambda i: (0, 0, i)), stat, stat],
        out_shape=[
            jax.ShapeDtypeStruct((nb, CPAD, m), BF16),
            jax.ShapeDtypeStruct((nb, m), F32),
            jax.ShapeDtypeStruct((nb, m), F32),
        ],
        scratch_shapes=[pltpu.VMEM((CPAD * (nb + ROW_GAP), lanes), F32)],
        compiler_params=params(),
        cost_estimate=cost(3e9, 4 * nb * CH * m),
        name="x_prep",
    )(x_gain, x_shift, x_cm)


def attn_fwd_kernel(base_ref, qp_ref, xn_ref, e_ref, ax_ref):
    xn = xn_ref[0]
    s = mm(qp_ref[...], xn)
    top = jnp.max(s, axis=1, keepdims=True)
    e = jnp.exp2(s - top)
    total = jnp.sum(e, axis=1, keepdims=True)
    e_low = e.astype(BF16)
    e_ref[0] = e_low
    ax = jnp.concatenate([mm_nt(e_low, xn), jnp.zeros((e.shape[0], AXW - CPAD), F32)], axis=1)
    lane = lax.broadcasted_iota(jnp.int32, ax.shape, 1)
    ax_ref[0] = jnp.where(lane == SUM_LANE, total, jnp.where(lane == MAX_LANE, top, ax))


def attn_fwd(base, qp, xn, half):
    n = qp.shape[0]
    m = xn.shape[2]
    return pl.pallas_call(
        attn_fwd_kernel,
        grid_spec=pltpu.PrefetchScalarGridSpec(
            num_scalar_prefetch=1,
            grid=(half,),
            in_specs=[
                pl.BlockSpec((n, CPAD), lambda i, base: (0, 0)),
                pl.BlockSpec((1, CPAD, m), lambda i, base: (base[0] + i, 0, 0)),
            ],
            out_specs=[
                pl.BlockSpec((1, n, m), lambda i, base: (i, 0, 0)),
                pl.BlockSpec((1, n, AXW), lambda i, base: (i, 0, 0)),
            ],
        ),
        out_shape=[
            jax.ShapeDtypeStruct((half, n, m), BF16),
            jax.ShapeDtypeStruct((half, n, AXW), F32),
        ],
        compiler_params=params(),
        cost_estimate=cost(4 * half * n * m * 512, half * n * m * 3),
        name="attn_fwd",
    )(base, qp, xn)


def combine(mine, other):
    top_a, top_b = mine[:, MAX_LANE:MAX_LANE + 1], other[:, MAX_LANE:MAX_LANE + 1]
    top = jnp.maximum(top_a, top_b)
    fa, fb = jnp.exp2(top_a - top), jnp.exp2(top_b - top)
    inv = 1.0 / (mine[:, SUM_LANE:SUM_LANE + 1] * fa + other[:, SUM_LANE:SUM_LANE + 1] * fb)
    ax = mine * (fa * inv) + other * (fb * inv)
    lane = lax.broadcasted_iota(jnp.int32, ax.shape, 1)
    return jnp.where(lane < CH, ax, 0.0), top, inv


def mlp_a_kernel(where_ref, axa_ref, axb_ref, z0_ref, wvo_ref, mg_ref, ms_ref, w1_ref, b1_ref, w2_ref, do_ref,
                 z1_ref, act_ref, dpre_ref, dw1_ref, dw2_ref, db1_ref):
    ax, _, _ = combine(axa_ref[0], axb_ref[0])
    z1 = z0_ref[...] + mm(ax[:, :CPAD].astype(BF16), wvo_ref[...])
    z1_ref[0] = z1
    h = layer_norm(z1, mg_ref[...], ms_ref[...]).astype(BF16)
    h_t = h.T
    d_out = do_ref[0]

    @pl.when(pl.program_id(0) == 0)
    def _():
        for ref in (dw1_ref, dw2_ref, db1_ref):
            ref[...] = jnp.zeros_like(ref)

    width = w1_ref.shape[1]
    step = 256
    for lo in range(0, width, step):
        cols = slice(lo, lo + step)
        pre = mm(h, w1_ref[:, cols]) + b1_ref[:, cols]
        d_act = mm_nt(d_out, w2_ref[cols, :]).astype(BF16).astype(F32)
        sq = pre * pre
        t = jnp.tanh(pre * (GELU_A + (GELU_A * GELU_B) * sq))
        half_t = 0.5 + 0.5 * t
        act = (pre * half_t).astype(BF16)
        slope = half_t + (0.5 * pre) * (1.0 - t * t) * (GELU_A + (3.0 * GELU_A * GELU_B) * sq)
        d_pre = d_act * slope
        db1_ref[:, cols] += jnp.sum(d_pre, axis=0, keepdims=True)
        d_pre_low = d_pre.astype(BF16)
        act_ref[0, :, cols] = act
        dpre_ref[0, :, cols] = d_pre_low
        dw1_ref[:, cols] += mm(h_t, d_pre_low)
        dw2_ref[cols, :] += mm(act.T, d_out)


def mlp_a(where, axa, axb, z0, wvo, mg, ms, w1, b1, w2, d_out):
    half, n, _ = axa.shape
    d = z0.shape[1]
    whole = lambda shape: pl.BlockSpec(shape, lambda i, base: (0,) * len(shape))
    per = lambda c: pl.BlockSpec((1, n, c), lambda i, base: (i, 0, 0))
    return pl.pallas_call(
        mlp_a_kernel,
        grid_spec=pltpu.PrefetchScalarGridSpec(
            num_scalar_prefetch=1,
            grid=(half,),
            in_specs=[per(AXW), per(AXW), whole((n, d)), whole((CPAD, d)), whole((1, d)), whole((1, d)),
                      whole((d, d)), whole((1, d)), whole((d, d)),
                      pl.BlockSpec((1, n, d), lambda i, base: (base[0] + i, 0, 0))],
            out_specs=[per(d), per(d), per(d), whole((d, d)), whole((d, d)), whole((1, d))],
        ),
        out_shape=[
            jax.ShapeDtypeStruct((half, n, d), F32),
            jax.ShapeDtypeStruct((half, n, d), BF16),
            jax.ShapeDtypeStruct((half, n, d), BF16),
            jax.ShapeDtypeStruct((d, d), F32),
            jax.ShapeDtypeStruct((d, d), F32),
            jax.ShapeDtypeStruct((1, d), F32),
        ],
        compiler_params=params(),
        cost_estimate=cost(2 * half * n * d * (4 * d + 512), half * n * d * 10),
        name="mlp_a",
    )(where, axa, axb, z0, wvo, mg, ms, w1, b1, w2, d_out)


def mlp_b_kernel(axa_ref, axb_ref, z1_ref, act_ref, dpre_ref, do_ref, wvo_ref, mg_ref, w1_ref, w2_ref, b2_ref, db1_ref, acc_in_ref,
                 z2_ref, full_ref, g_ref, acc_ref):
    ax, top, inv = combine(axa_ref[0], axb_ref[0])
    n, _ = z1_ref.shape[1:]
    z1 = z1_ref[0]
    z2 = z1 + mm(act_ref[0], w2_ref[...]) + b2_ref[...]
    z2_ref[0] = z2
    full_ref[0] = z2
    d_hid = mm_nt(dpre_ref[0], w1_ref[...]).astype(BF16).astype(F32)
    centred = z1 - jnp.mean(z1, axis=1, keepdims=True)
    rstd = lax.rsqrt(jnp.mean(centred * centred, axis=1, keepdims=True) + LN_EPS)
    hat = centred * rstd
    d_hat = d_hid * mg_ref[...]
    mean_a = jnp.mean(d_hat, axis=1, keepdims=True)
    mean_b = jnp.mean(d_hat * hat, axis=1, keepdims=True)
    d_out = do_ref[0].astype(F32)
    d_mid = d_out + rstd * (d_hat - mean_a - hat * mean_b)
    d_mid_low = d_mid.astype(BF16)

    @pl.when(pl.program_id(0) == 0)
    def _():
        acc_ref[...] = jnp.zeros_like(acc_ref) if acc_in_ref is None else acc_in_ref[...]
        if acc_in_ref is None:
            acc_ref[VEC_ROW + 3:VEC_ROW + 4, :] = db1_ref[...]

    p = mm(ax[:, :CPAD].astype(BF16).T, d_mid_low)
    acc_ref[0:n, :] += d_mid
    acc_ref[n:n + CPAD, :] += p
    acc_ref[VEC_ROW:VEC_ROW + 1, :] += jnp.sum(d_hid * hat, axis=0, keepdims=True)
    acc_ref[VEC_ROW + 1:VEC_ROW + 2, :] += jnp.sum(d_hid, axis=0, keepdims=True)
    acc_ref[VEC_ROW + 2:VEC_ROW + 3, :] += jnp.sum(d_out, axis=0, keepdims=True)
    d_ax = jnp.concatenate([mm_nt(d_mid_low, wvo_ref[...]), jnp.zeros((n, AXW - CPAD), F32)], axis=1)
    delta = jnp.sum(d_ax * ax, axis=1, keepdims=True)
    lane = lax.broadcasted_iota(jnp.int32, d_ax.shape, 1)
    g_ref[0] = jnp.where(lane == SUM_LANE, delta, jnp.where(lane == MAX_LANE, top, jnp.where(lane == INV_LANE, inv, d_ax)))


def mlp_b(base, axa, axb, z1, act, dpre, d_out, wvo, mg, w1, w2, b2, db1, start, count, acc_in, full_in):
    n = axa.shape[1]
    d = z1.shape[2]
    whole = lambda shape: pl.BlockSpec(shape, lambda i, base: (0,) * len(shape))
    part = lambda c: pl.BlockSpec((1, n, c), lambda i, base: (i + start, 0, 0))
    per = lambda c: pl.BlockSpec((1, n, c), lambda i, base: (i, 0, 0))
    shifted = pl.BlockSpec((1, n, d), lambda i, base: (base[0] + start + i, 0, 0))
    in_specs = [part(AXW), part(AXW), part(d), part(d), part(d), shifted, whole((CPAD, d)), whole((1, d)),
                whole((d, d)), whole((d, d)), whole((1, d)), whole((1, d))]
    args = [axa, axb, z1, act, dpre, d_out, wvo, mg, w1, w2, b2, db1]
    aliases = {}
    if acc_in is not None:
        in_specs += [whole((ACC_ROWS, d)), pl.BlockSpec(memory_space=pl.ANY)]
        args += [acc_in, full_in]
        aliases = {14: 1}

    def body(base_ref, *refs):
        mlp_b_kernel(*refs[:12], refs[12] if acc_in is not None else None, *refs[-4:])

    return pl.pallas_call(
        body,
        grid_spec=pltpu.PrefetchScalarGridSpec(
            num_scalar_prefetch=1,
            grid=(count,),
            in_specs=in_specs,
            out_specs=[per(d), shifted, per(AXW), whole((ACC_ROWS, d))],
        ),
        out_shape=[
            jax.ShapeDtypeStruct((count, n, d), F32),
            jax.ShapeDtypeStruct(d_out.shape, F32),
            jax.ShapeDtypeStruct((count, n, AXW), F32),
            jax.ShapeDtypeStruct((ACC_ROWS, d), F32),
        ],
        input_output_aliases=aliases,
        compiler_params=params(),
        cost_estimate=cost(2 * count * n * d * (2 * d + 800), count * n * d * 18),
        name="mlp_b",
    )(base, *args)


def places():
    core, chip = lax.axis_index('cp'), lax.axis_index('dp')
    x, y = lax.rem(chip, 2), chip // 2
    at_x = (y * 2 + (1 - x), core)
    at_y = ((1 - y) * 2 + x, core)
    return core, x, y, (chip, 1 - core), at_x, at_y


def meet(devices):
    barrier = pltpu.get_barrier_semaphore()
    for dev in devices:
        pl.semaphore_signal(barrier, inc=1, device_id=dev, device_id_type=pl.DeviceIdType.MESH)
    pl.semaphore_wait(barrier, len(devices))


def remote(src, dst, sems, k, dev):
    return pltpu.make_async_remote_copy(
        src_ref=src, dst_ref=dst, send_sem=sems[0].at[k], recv_sem=sems[1].at[k],
        device_id=dev, device_id_type=pl.DeviceIdType.MESH)


def rows(ref, start, size):
    return ref.at[pl.ds(pl.multiple_of(start, 8), size)]


def scatter_step(step, acc_ref, piece_ref, half_ref, rx0_ref, rx1_ref, rx2_ref, sems):
    half, quarter, eighth, part = (ACC_ROWS // k for k in (2, 4, 8, 16))
    core, x, y, at_core, at_x, at_y = places()
    p0 = remote(rows(acc_ref, (1 - core) * half, half), rx0_ref, sems, 0, at_core)
    p1a = remote(rows(half_ref, (1 - x) * eighth, eighth), rx1_ref.at[0], sems, 1, at_x)
    p1b = remote(rows(half_ref, quarter + (1 - y) * eighth, eighth), rx1_ref.at[1], sems, 2, at_y)
    a, b = x * eighth, quarter + y * eighth
    p2a = remote(rows(half_ref, a + (1 - y) * part, part), rx2_ref.at[0], sems, 3, at_y)
    p2b = remote(rows(half_ref, b + (1 - x) * part, part), rx2_ref.at[1], sems, 4, at_x)

    @pl.when(step == 0)
    def _():
        meet((at_core, at_x, at_y))
        p0.start()

    @pl.when(step == 2)
    def _():
        p0.wait()
        half_ref[...] = acc_ref[pl.ds(pl.multiple_of(core * half, 8), half), :] + rx0_ref[...]
        p1a.start()
        p1b.start()

    @pl.when(step == 5)
    def _():
        p1a.wait()
        p1b.wait()
        half_ref[pl.ds(pl.multiple_of(a, 8), eighth), :] += rx1_ref[0]
        half_ref[pl.ds(pl.multiple_of(b, 8), eighth), :] += rx1_ref[1]
        p2a.start()
        p2b.start()

    @pl.when(step == 7)
    def _():
        p2a.wait()
        p2b.wait()
        piece_ref[0] = half_ref[pl.ds(pl.multiple_of(a + y * part, 8), part), :] + rx2_ref[0]
        piece_ref[1] = half_ref[pl.ds(pl.multiple_of(b + x * part, 8), part), :] + rx2_ref[1]


def gather_step(step, piece_ref, out_ref, buf_ref, sems):
    half, quarter, eighth, part = (ACC_ROWS // k for k in (2, 4, 8, 16))
    core, x, y, at_core, at_x, at_y = places()
    own = core * half
    a, b = own + x * eighth, own + quarter + y * eighth

    def spread(start, size, k, dev):
        return remote(rows(buf_ref, start, size), rows(buf_ref, start, size), sems, k, dev)

    p3a = remote(piece_ref.at[0], rows(buf_ref, a + y * part, part), sems, 0, at_y)
    p3b = remote(piece_ref.at[1], rows(buf_ref, b + x * part, part), sems, 1, at_x)
    p4a = spread(a, eighth, 2, at_x)
    p4b = spread(b, eighth, 3, at_y)
    p5 = spread(own, half, 4, at_core)

    @pl.when(step == 0)
    def _():
        buf_ref[pl.ds(pl.multiple_of(a + y * part, 8), part), :] = piece_ref[0]
        buf_ref[pl.ds(pl.multiple_of(b + x * part, 8), part), :] = piece_ref[1]
        meet((at_core, at_x, at_y))
        p3a.start()
        p3b.start()

    @pl.when(step == 2)
    def _():
        p3a.wait()
        p3b.wait()
        p4a.start()
        p4b.start()

    @pl.when(step == 6)
    def _():
        p4a.wait()
        p4b.wait()
        p5.start()

    @pl.when(step == 7)
    def _():
        p5.wait()
        out_ref[...] = buf_ref[...]


def attn_bwd_body(ga_ref, gb_ref, ax_ref, e_ref, xn_ref, qpt_ref, t_in_ref, dxn_ref, t_ref):
    g = jnp.where(pl.program_id(0) < pl.num_programs(0) // 2, ga_ref[0], gb_ref[0])
    xn = xn_ref[0]
    e = e_ref[0]
    beta = jnp.exp2(ax_ref[0][:, MAX_LANE:MAX_LANE + 1] - g[:, MAX_LANE:MAX_LANE + 1]) * g[:, INV_LANE:INV_LANE + 1]
    lane = lax.broadcasted_iota(jnp.int32, g.shape, 1)
    scaled = g * beta
    d_low = jnp.where(lane < CH, scaled, 0.0)[:, :CPAD].astype(BF16)
    d_a = mm(d_low, xn)
    d_s = (e.astype(F32) * (d_a - scaled[:, SUM_LANE:SUM_LANE + 1])).astype(BF16)

    @pl.when(pl.program_id(0) == 0)
    def _():
        t_ref[...] = t_in_ref[...]

    t_ref[...] += mm_nt(xn, d_s)
    dxn_ref[0] = (mm(qpt_ref[...], d_s) + mm(d_low.T, e)).astype(BF16)


def bwd_scatter_kernel(*refs):
    step = pl.program_id(0)
    sems = refs[15:17]
    scatter_step(step, refs[7], refs[10], *refs[11:15], sems)
    attn_bwd_body(*refs[:7], *refs[8:10])


def bwd_gather_kernel(*refs):
    step = pl.program_id(0)
    sems = refs[13:15]
    gather_step(step, refs[7], refs[11], refs[12], sems)
    attn_bwd_body(*refs[:7], *refs[9:11])


def attn_bwd(own, ga, gb, ax, e, xn, qpt, t_in, travel, dxn_in):
    half, n, m = e.shape
    width = travel.shape[-1]
    whole = lambda shape: pl.BlockSpec(shape, lambda i: (0,) * len(shape))
    per = lambda c: pl.BlockSpec((1, n, c), lambda i: (i, 0, 0))

    def at(i):
        core = lax.axis_index('cp')
        return ((core if own else 1 - core) * half + i, 0, 0)

    shifted = pl.BlockSpec((1, CPAD, m), at)
    first = pl.BlockSpec((1, n, AXW), lambda i: (jnp.minimum(i, half // 2 - 1), 0, 0))
    second = pl.BlockSpec((1, n, AXW), lambda i: (jnp.maximum(i - half // 2, 0), 0, 0))
    in_specs = [first, second, per(AXW), per(m), shifted, whole((CPAD, n)), whole((CPAD, n)), whole(travel.shape)]
    out_specs = [shifted, whole((CPAD, n))]
    out_shape = [jax.ShapeDtypeStruct(xn.shape, BF16), jax.ShapeDtypeStruct((CPAD, n), F32)]
    args = [ga, gb, ax, e, xn, qpt, t_in, travel]
    eighth, part = ACC_ROWS // 8, ACC_ROWS // 16
    if own:
        kernel, aliases, count, ident = bwd_scatter_kernel, {}, 5, 1
        out_specs.append(whole((2, part, width)))
        out_shape.append(jax.ShapeDtypeStruct((2, part, width), F32))
        scratch = [pltpu.VMEM((ACC_ROWS // 2, width), F32), pltpu.VMEM((ACC_ROWS // 2, width), F32),
                   pltpu.VMEM((2, eighth, width), F32), pltpu.VMEM((2, part, width), F32)]
    else:
        kernel, aliases, count, ident = bwd_gather_kernel, {8: 0}, 5, 2
        in_specs.append(pl.BlockSpec(memory_space=pl.ANY))
        args.append(dxn_in)
        out_specs.append(whole((ACC_ROWS, width)))
        out_shape.append(jax.ShapeDtypeStruct((ACC_ROWS, width), F32))
        scratch = [pltpu.VMEM((ACC_ROWS, width), F32)]
    scratch += [pltpu.SemaphoreType.DMA((count,)), pltpu.SemaphoreType.DMA((count,))]
    return pl.pallas_call(
        kernel,
        grid=(half,),
        in_specs=in_specs,
        out_specs=out_specs,
        out_shape=out_shape,
        scratch_shapes=scratch,
        input_output_aliases=aliases,
        compiler_params=pltpu.CompilerParams(
            vmem_limit_bytes=VMEM_LIMIT, dimension_semantics=("arbitrary",), collective_id=ident, has_side_effects=True),
        cost_estimate=cost(8 * half * n * m * 512, half * n * m * 6),
        name="attn_bwd",
    )(*args)


def x_post_kernel(base_ref, gain_ref, x_ref, mean_ref, rstd_ref, dxn_ref, z2a_ref, z2b_ref, full_in_ref, dx_ref, sums_ref, full_ref,
                  rows_ref, dg_ref, ds_ref):
    nb, lanes = x_ref.shape[1:]
    pitch = CPAD + ROW_GAP
    early = pl.program_id(0) < pl.num_programs(0) // 2

    @pl.when(early)
    def _():
        full_ref[0] = z2a_ref[0]

    @pl.when(jnp.logical_not(early))
    def _():
        full_ref[0] = z2b_ref[0]

    for b in range(nb):
        rows_ref[b * pitch:b * pitch + CPAD, :] = dxn_ref[b].astype(F32)
    zero = jnp.zeros((nb, lanes), F32)
    mean = mean_ref[...]
    rstd = rstd_ref[...]

    @pl.when(pl.program_id(0) == 0)
    def _():
        dg_ref[...] = jnp.zeros_like(dg_ref)
        ds_ref[...] = jnp.zeros_like(ds_ref)

    def gather(c, acc):
        da, db = acc
        hat = (x_ref[c].astype(F32) - mean) * rstd
        dxn = rows_ref[pl.ds(c, nb, stride=pitch), :]
        dh = dxn * gain_ref[c]
        prod = dxn * hat
        dg_ref[c] += prod[:8] + prod[8:]
        ds_ref[c] += dxn[:8] + dxn[8:]
        return da + dh, db + dh * hat

    da, db = lax.fori_loop(0, CH, gather, (zero, zero), unroll=9)
    mean_a = da * (1.0 / CH)
    mean_b = db * (1.0 / CH)

    def put(c, carry):
        hat = (x_ref[c].astype(F32) - mean) * rstd
        dxn = rows_ref[pl.ds(c, nb, stride=pitch), :]
        dx_ref[c] = (rstd * (dxn * gain_ref[c] - mean_a - hat * mean_b)).astype(BF16)
        return carry

    lax.fori_loop(0, CH, put, 0, unroll=9)

    @pl.when(pl.program_id(0) == pl.num_programs(0) - 1)
    def _():
        for k, ref in enumerate((dg_ref, ds_ref)):
            part = jnp.concatenate([jnp.sum(ref[...], axis=1), jnp.zeros((AXW - CH, lanes), F32)], axis=0)
            sums_ref[k:k + 1, :] = jnp.sum(part.T, axis=0, keepdims=True)


def x_post(base, x_gain, x_cm, mean, rstd, dxn, z2a, z2b, full):
    _, nb, m = x_cm.shape
    part, n, d = z2a.shape
    half = 2 * part
    lanes = m // half
    whole = lambda shape: pl.BlockSpec(shape, lambda i, base: (0,) * len(shape))
    chan = pl.BlockSpec((CH, nb, lanes), lambda i, base: (0, 0, i))
    stat = pl.BlockSpec((nb, lanes), lambda i, base: (0, i))
    return pl.pallas_call(
        x_post_kernel,
        grid_spec=pltpu.PrefetchScalarGridSpec(
            num_scalar_prefetch=1,
            grid=(half,),
            in_specs=[
                pl.BlockSpec(memory_space=pltpu.SMEM),
                chan, stat, stat,
                pl.BlockSpec((nb, CPAD, lanes), lambda i, base: (0, 0, i)),
                pl.BlockSpec((1, n, d), lambda i, base: (jnp.minimum(i, part - 1), 0, 0)),
                pl.BlockSpec((1, n, d), lambda i, base: (jnp.maximum(i - part, 0), 0, 0)),
                pl.BlockSpec(memory_space=pl.ANY),
            ],
            out_specs=[chan, whole((2, AXW)), pl.BlockSpec((1, n, d), lambda i, base: (base[0] + i, 0, 0))],
            scratch_shapes=[pltpu.VMEM(((CPAD + ROW_GAP) * nb, lanes), F32),
                            pltpu.VMEM((CH, 8, lanes), F32), pltpu.VMEM((CH, 8, lanes), F32)],
        ),
        out_shape=[
            jax.ShapeDtypeStruct(x_cm.shape, BF16),
            jax.ShapeDtypeStruct((2, AXW), F32),
            jax.ShapeDtypeStruct(full.shape, F32),
        ],
        input_output_aliases={8: 2},
        compiler_params=params(),
        cost_estimate=cost(6e9, 6 * nb * CH * m + 8 * half * n * d),
        name="x_post",
    )(base, x_gain, x_cm, mean, rstd, dxn, z2a, z2b, full)


def small_sum_kernel(devices, x_ref, o_ref, got_ref, send_sem, recv_sem):
    dp, cp = devices
    my_dp, my_cp = lax.axis_index('dp'), lax.axis_index('cp')
    barrier = pltpu.get_barrier_semaphore()
    peers = [(i, j) for i in range(dp) for j in range(cp)][1:]
    ids = [(lax.rem(my_dp + i, dp), lax.rem(my_cp + j, cp)) for i, j in peers]
    for dev in ids:
        pl.semaphore_signal(barrier, inc=1, device_id=dev, device_id_type=pl.DeviceIdType.MESH)
    pl.semaphore_wait(barrier, len(ids))
    copies = []
    for k, dev in enumerate(ids):
        copies.append(pltpu.make_async_remote_copy(
            src_ref=x_ref, dst_ref=got_ref.at[k], send_sem=send_sem.at[k], recv_sem=recv_sem.at[k],
            device_id=dev, device_id_type=pl.DeviceIdType.MESH))
        copies[-1].start()
    for copy in copies:
        copy.wait()
    o_ref[...] = x_ref[...] + jnp.sum(got_ref[...], axis=0)


def small_sum(mesh, x):
    count = mesh.size - 1
    return pl.pallas_call(
        functools.partial(small_sum_kernel, (mesh.shape['dp'], mesh.shape['cp'])),
        in_specs=[pl.BlockSpec(memory_space=pltpu.VMEM)],
        out_specs=pl.BlockSpec(memory_space=pltpu.VMEM),
        out_shape=jax.ShapeDtypeStruct(x.shape, F32),
        scratch_shapes=[pltpu.VMEM((count,) + x.shape, F32),
                        pltpu.SemaphoreType.DMA((count,)), pltpu.SemaphoreType.DMA((count,))],
        compiler_params=pltpu.CompilerParams(collective_id=0, has_side_effects=True),
        name="small_sum",
    )(x)


def solution(mesh):
    x_spec = P('dp', 'cp', None)
    row_spec = P('dp', None, None)
    vec_spec = P(None)
    mat_spec = P(None, None)
    in_specs = (x_spec, mat_spec, vec_spec, vec_spec, vec_spec, vec_spec, mat_spec, mat_spec, mat_spec, mat_spec,
                vec_spec, vec_spec, mat_spec, vec_spec, mat_spec, vec_spec, row_spec)
    out_specs = (row_spec, x_spec, mat_spec, vec_spec, vec_spec, vec_spec, vec_spec, mat_spec, mat_spec, mat_spec, mat_spec,
                 vec_spec, vec_spec, mat_spec, vec_spec, mat_spec, vec_spec)
    swap = [(0, 1), (1, 0)]

    def step(inputs, latents, x_gain, x_shift, z_gain, z_shift, w_query, w_key, w_value, w_out, m_gain, m_shift, w_up, b_up, w_down, b_down, d_out):
        qk_scale = w_query.shape[1] ** -0.5
        n, d = latents.shape
        half = inputs.shape[0] // 2
        core = lax.axis_index('cp')
        as_ints = lambda *vals: jnp.stack([v.astype(jnp.int32) for v in vals])
        mine = as_ints(core * half, core * (d // 2))
        other = as_ints((1 - core) * half, (1 - core) * (d // 2))
        row = lambda vec: vec.reshape(1, -1)

        def both(own, axis):
            got = lax.ppermute(own, 'cp', swap)
            return jnp.where(core == 0, jnp.concatenate([own, got], axis), jnp.concatenate([got, own], axis))

        x_cm = jnp.transpose(inputs, (2, 0, 1))
        xn, x_mean, x_rstd = x_prep(x_cm, x_gain, x_shift)

        z_ln, z_pull = jax.vjp(layer_norm, latents, z_gain, z_shift)
        z_norm = z_ln.astype(BF16)
        queries = mm(z_norm, w_query).astype(BF16)
        wk_pad = jnp.pad(w_key, ((0, CPAD - CH), (0, 0)))
        q_key = mm_nt(queries, wk_pad)
        qp = (q_key * (qk_scale * LOG2E)).astype(BF16)
        qpt = (mm_nt(wk_pad, queries) * qk_scale).astype(BF16)
        wvo = mm(jnp.pad(w_value, ((0, CPAD - CH), (0, 0))), w_out).astype(BF16)

        e_other, ax_other = attn_fwd(other, qp, xn, half)
        ax_got = lax.ppermute(ax_other, 'cp', swap)
        e_mine, ax_mine = attn_fwd(mine, qp, xn, half)

        z1, act, dpre, dw1, dw2, db1 = mlp_a(
            mine, ax_mine, ax_got, latents, wvo, row(m_gain), row(m_shift), w_up, row(b_up), w_down, d_out)
        d_w_up, d_w_down = lax.psum((dw1, dw2), ('dp', 'cp'))
        mlp_args = (mine, ax_mine, ax_got, z1, act, dpre, d_out, wvo, row(m_gain), w_up, w_down, row(b_down), db1)
        z2a, full, ga, acc = mlp_b(*mlp_args, 0, half // 2, None, None)
        ga_got = lax.ppermute(ga, 'cp', swap)
        z2a_got = lax.ppermute(z2a, 'cp', swap)
        z2b, full, gb, acc = mlp_b(*mlp_args, half // 2, half // 2, acc, full)
        gb_got = lax.ppermute(gb, 'cp', swap)
        dxn, t_part, piece = attn_bwd(
            True, ga, gb, ax_mine, e_mine, xn, qpt, jnp.zeros((CPAD, n), F32), acc, None)
        z2b, dxn = lax.optimization_barrier((z2b, dxn))
        z2b_got = lax.ppermute(z2b, 'cp', swap)
        dxn, t_part, acc = attn_bwd(
            False, ga_got, gb_got, ax_other, e_other, xn, qpt, t_part, piece, dxn)

        t_mine = lax.dynamic_slice_in_dim(t_part, core * (CPAD // 2), CPAD // 2, 0)
        t_send = lax.dynamic_slice_in_dim(t_part, (1 - core) * (CPAD // 2), CPAD // 2, 0)
        t_mine = t_mine + lax.ppermute(t_send, 'cp', swap)
        t_parts = [t_mine]
        for bit in (1, 2, 3):
            t_parts.append(lax.ppermute(t_mine, 'dp', [(k, k ^ bit) for k in range(4)]))
        dx_cm, sums, z_out = x_post(other, x_gain, x_cm, x_mean, x_rstd, dxn, z2a_got, z2b_got, full)
        t_sum = both((t_parts[0] + t_parts[1]) + (t_parts[2] + t_parts[3]), 0)
        sums = small_sum(mesh, sums)
        d_x_gain, d_x_shift = sums[0, :CH], sums[1, :CH]

        d_mid_sum = acc[:n]
        p_low = acc[n:n + CH].astype(BF16)
        d_m_gain, d_m_shift, d_b_down, d_b_up = (acc[VEC_ROW + k] for k in range(4))
        d_w_out = mm_tn(w_value, p_low)
        d_w_value = mm_nt(p_low, w_out)
        t_low = (t_sum[:CH] * qk_scale).astype(BF16)
        d_query = mm_tn(t_low, w_key).astype(BF16)
        d_w_key = mm(t_low, queries)
        d_z_norm = mm_nt(d_query, w_query)
        d_w_query = mm_tn(z_norm, d_query)
        d_lat_ln, d_z_gain, d_z_shift = z_pull(d_z_norm)
        return (z_out, jnp.transpose(dx_cm, (1, 2, 0)), d_lat_ln + d_mid_sum, d_x_gain, d_x_shift, d_z_gain, d_z_shift,
                d_w_query, d_w_key, d_w_value, d_w_out, d_m_gain, d_m_shift, d_w_up, d_b_up, d_w_down, d_b_down)

    return jax.shard_map(step, mesh=mesh, in_specs=in_specs, out_specs=out_specs, check_vma=False)
```

```python
import functools
import math

import jax
import jax.numpy as jnp
from jax import lax
from jax.experimental import pallas as pl
from jax.experimental.pallas import tpu as pltpu
from jax.sharding import PartitionSpec as P


LN_EPS = 1e-5
F32 = jnp.float32
BF16 = jnp.bfloat16
CH = 261
CPAD = 272
AXW = 384
ROW_GAP = 8
ACC_ROWS = 896
VEC_ROW = 784
SUM_LANE = 261
MAX_LANE = 262
INV_LANE = 263
LOG2E = math.log2(math.e)
GELU_A = math.sqrt(2.0 / math.pi)
GELU_B = 0.044715
VMEM_LIMIT = 63 * 1024 * 1024


def layer_norm(tensor, ln_gain, ln_shift):
    row_mean = jnp.mean(tensor, axis=-1, keepdims=True)
    centred = tensor - row_mean
    variance = jnp.mean(centred * centred, axis=-1, keepdims=True)
    return centred * lax.rsqrt(variance + LN_EPS) * ln_gain + ln_shift


def mm(lhs, rhs):
    return lax.dot_general(lhs, rhs, (((1,), (0,)), ((), ())), preferred_element_type=F32)


def mm_nt(lhs, rhs):
    return lax.dot_general(lhs, rhs, (((1,), (1,)), ((), ())), preferred_element_type=F32)


def params(semantics=1):
    return pltpu.CompilerParams(
        vmem_limit_bytes=VMEM_LIMIT, dimension_semantics=("arbitrary",) * semantics)


def whole(shape, **kw):
    return pl.BlockSpec(shape, lambda *_: (0,) * len(shape), **kw)


def once(shape):
    return whole(shape, pipeline_mode=pl.Buffered(1))


def lead(shape, index=lambda i: i):
    return pl.BlockSpec(shape, lambda i, *_: (index(i),) + (0,) * (len(shape) - 1))


def trail(shape):
    return pl.BlockSpec(shape, lambda i, *_: (0,) * (len(shape) - 1) + (i,))


def column(array, lane):
    return array[:, lane:lane + 1]


def cost(flops, nbytes):
    return pl.CostEstimate(flops=int(flops), bytes_accessed=int(nbytes), transcendentals=0)


def x_prep_kernel(gain_ref, shift_ref, x_ref, xn_ref, mean_ref, rstd_ref, rows_ref):
    nb = x_ref.shape[1]
    lanes = x_ref.shape[2]
    pitch = nb + ROW_GAP
    zero = jnp.zeros((nb, lanes), F32)

    def add_up(c, acc):
        return acc + x_ref[c].astype(F32)

    mean = lax.fori_loop(0, CH, add_up, zero, unroll=9) * (1.0 / CH)

    def add_sq(c, acc):
        d = x_ref[c].astype(F32) - mean
        return acc + d * d

    var = lax.fori_loop(0, CH, add_sq, zero, unroll=9) * (1.0 / CH)
    rstd = lax.rsqrt(var + LN_EPS)
    mean_ref[:] = mean
    rstd_ref[:] = rstd

    def put(c, carry):
        xn = (x_ref[c].astype(F32) - mean) * rstd * gain_ref[c] + shift_ref[c]
        rows_ref[pl.ds(pl.multiple_of(c * pitch, ROW_GAP), nb), :] = xn
        return carry

    lax.fori_loop(0, CH, put, 0, unroll=9)
    rows_ref[CH * pitch:CPAD * pitch, :] = jnp.zeros(((CPAD - CH) * pitch, lanes), F32)
    for b in range(nb):
        xn_ref[b] = rows_ref[pl.ds(b, CPAD, stride=pitch), :].astype(BF16)


def x_prep(x_cm, x_gain, x_shift):
    _, nb, m = x_cm.shape
    lanes = 128
    stat = trail((nb, lanes))
    return pl.pallas_call(
        x_prep_kernel,
        grid=(m // lanes,),
        in_specs=[
            pl.BlockSpec(memory_space=pltpu.SMEM),
            pl.BlockSpec(memory_space=pltpu.SMEM),
            trail((CH, nb, lanes)),
        ],
        out_specs=[trail((nb, CPAD, lanes)), stat, stat],
        out_shape=[
            jax.ShapeDtypeStruct((nb, CPAD, m), BF16),
            jax.ShapeDtypeStruct((nb, m), F32),
            jax.ShapeDtypeStruct((nb, m), F32),
        ],
        scratch_shapes=[pltpu.VMEM((CPAD * (nb + ROW_GAP), lanes), F32)],
        compiler_params=params(),
        cost_estimate=cost(3e9, 4 * nb * CH * m),
        name="x_prep",
    )(x_gain, x_shift, x_cm)


def attn_fwd_kernel(base_ref, qp_ref, xn_ref, e_ref, ax_ref):
    xn = xn_ref[0]
    n = qp_ref.shape[0]
    spans = [slice(k * (n // 2), (k + 1) * (n // 2)) for k in range(2)]
    logits = [mm(qp_ref[span, :], xn) for span in spans]
    for span, s in zip(spans, logits):
        top = jnp.max(s, axis=1, keepdims=True)
        e = jnp.exp2(s - top)
        total = jnp.sum(e, axis=1, keepdims=True)
        e_low = e.astype(BF16)
        e_ref[0, span, :] = e_low
        ax = jnp.concatenate([mm_nt(e_low, xn), jnp.zeros((e.shape[0], AXW - CPAD), F32)], axis=1)
        lane = lax.broadcasted_iota(jnp.int32, ax.shape, 1)
        ax_ref[0, span, :] = jnp.where(lane == SUM_LANE, total, jnp.where(lane == MAX_LANE, top, ax))


def attn_fwd(base, qp, xn, half):
    n = qp.shape[0]
    m = xn.shape[2]
    return pl.pallas_call(
        attn_fwd_kernel,
        grid_spec=pltpu.PrefetchScalarGridSpec(
            num_scalar_prefetch=1,
            grid=(half,),
            in_specs=[
                whole((n, CPAD)),
                pl.BlockSpec((1, CPAD, m), lambda i, base: (base[0] + i, 0, 0)),
            ],
            out_specs=[
                lead((1, n, m)),
                lead((1, n, AXW)),
            ],
        ),
        out_shape=[
            jax.ShapeDtypeStruct((half, n, m), BF16),
            jax.ShapeDtypeStruct((half, n, AXW), F32),
        ],
        compiler_params=params(),
        cost_estimate=cost(4 * half * n * m * 512, half * n * m * 3),
        name="attn_fwd",
    )(base, qp, xn)


def places():
    core, chip = lax.axis_index('cp'), lax.axis_index('dp')
    x, y = lax.rem(chip, 2), chip // 2
    at_x = (y * 2 + (1 - x), core)
    at_y = ((1 - y) * 2 + x, core)
    return core, x, y, (chip, 1 - core), at_x, at_y


def meet(devices):
    barrier = pltpu.get_barrier_semaphore()
    for dev in devices:
        pl.semaphore_signal(barrier, inc=1, device_id=dev, device_id_type=pl.DeviceIdType.MESH)
    pl.semaphore_wait(barrier, len(devices))


def remote(src, dst, sems, k, dev):
    return pltpu.make_async_remote_copy(
        src_ref=src, dst_ref=dst, send_sem=sems[0].at[k], recv_sem=sems[1].at[k],
        device_id=dev, device_id_type=pl.DeviceIdType.MESH)


def rows(ref, start, size):
    return ref.at[pl.ds(pl.multiple_of(start, 8), size)]


def take(ref, start, size):
    return ref[pl.ds(pl.multiple_of(start, 8), size), :]


def at_step(step, when, todo):
    pl.when(step == when)(todo)


def dma_sems(count):
    return [pltpu.SemaphoreType.DMA((count,)), pltpu.SemaphoreType.DMA((count,))]


class Carry:
    def __init__(self, in_shape, in_hbm, out_shape, scratch, head, tail, out_hbm=False):
        self.in_shape, self.in_hbm, self.out_shape, self.scratch = in_shape, in_hbm, out_shape, scratch
        self.out_hbm = out_hbm
        self.head, self.tail = head, tail


def start_all(copies):
    for copy in copies:
        copy.start()


def wait_all(copies):
    for copy in copies:
        copy.wait()


class Plan:
    def __init__(self, total):
        self.half, self.quarter, self.eighth, self.part = (total // k for k in (2, 4, 8, 16))
        self.core, self.x, self.y, self.at_core, self.at_x, self.at_y = places()
        self.spot = (self.x * self.eighth, self.quarter + self.y * self.eighth)
        self.away = ((1 - self.x) * self.eighth, self.quarter + (1 - self.y) * self.eighth)
        self.fine = (self.y * self.part, self.x * self.part)
        self.fine_away = ((1 - self.y) * self.part, (1 - self.x) * self.part)
        self.first, self.second = (self.at_x, self.at_y), (self.at_y, self.at_x)


def carry(total, width, stages, at):
    half, _, eighth, part = (total // k for k in (2, 4, 8, 16))
    lo, hi = stages[0], stages[-1]
    in_shape = {0: (total, width), 1: (half, width), 2: (2, eighth, width), 3: (2, part, width)}[lo]
    out_shape = {0: (half, width), 1: (2, eighth, width), 2: (2, part, width), 3: (2, eighth, width), 4: (half, width)}[hi]
    shapes = {}
    if 0 in stages:
        shapes.update(half=(half, width), rx0=(half, width))
    if 1 in stages:
        shapes.update(rx1=(2, eighth, width))
    if 2 in stages:
        shapes.update(rx2=(2, part, width))
    if 1 in stages and 2 in stages:
        shapes.update(mid=(2, eighth, width))
    if 2 in stages and 3 in stages:
        shapes.update(fin=(2, part, width))
    if 3 in stages:
        shapes.update(buf=(2, eighth, width))
    if 4 in stages:
        shapes.update(full=(half, width))
    names = list(shapes)
    count = 2 * len(stages)
    scratch = [pltpu.VMEM(shape, F32) for shape in shapes.values()] + [pltpu.SemaphoreType.DMA((1,))] + dma_sems(count)

    def build(src, refs):
        r = dict(zip(names, refs))
        local, sems = refs[-3], (refs[-2], refs[-1])
        p = Plan(total)
        slot = lambda stage, k: 2 * (stage - lo) + k
        two = (0, 1)
        moves = {}
        if 0 in stages:
            moves[0] = lambda: [pltpu.make_async_copy(rows(src, p.core * half, half), r['half'], local.at[0]),
                                remote(rows(src, (1 - p.core) * half, half), r['rx0'], sems, slot(0, 0), p.at_core)]
        if 1 in stages:
            pair = r.get('half', src)
            moves[1] = lambda: [remote(rows(pair, p.away[k], eighth), r['rx1'].at[k], sems, slot(1, k), p.first[k])
                                for k in two]
        if 2 in stages:
            mid = r.get('mid', src)
            moves[2] = lambda: [remote(rows(mid.at[k], p.fine_away[k], part), r['rx2'].at[k], sems, slot(2, k), p.second[k])
                                for k in two]
        if 3 in stages:
            fin = r.get('fin', src)
            moves[3] = lambda: [remote(fin.at[k], rows(r['buf'].at[k], p.fine[k], part), sems, slot(3, k), p.second[k])
                                for k in two]
        if 4 in stages:
            moves[4] = lambda: [remote(r['buf'].at[k], rows(r['full'], p.spot[k], eighth), sems, slot(4, k), p.first[k])
                                for k in two]

        def before(stage):
            if stage == 3:
                for k in two:
                    r['buf'][k, pl.ds(pl.multiple_of(p.fine[k], 8), part), :] = fin[k]

        def after(stage, out):
            wait_all(moves[stage]())
            if stage == 0:
                r['half'][:] += r['rx0'][:]
                if hi == 0:
                    out[:] = r['half'][:]
            elif stage == 1:
                dst = out if hi == 1 else r['mid']
                for k in two:
                    dst[k] = take(pair, p.spot[k], eighth) + r['rx1'][k]
            elif stage == 2:
                dst = out if hi == 2 else r['fin']
                for k in two:
                    dst[k] = take(mid.at[k], p.fine[k], part) + r['rx2'][k]
            elif stage == 3 and hi == 3:
                out[:] = r['buf'][:]
            elif stage == 4:
                for k in two:
                    r['full'][pl.ds(pl.multiple_of(p.spot[k], 8), eighth), :] = r['buf'][k]
                out[:] = r['full'][:]

        return moves, before, after

    def head(step, src, out, refs):
        for stage, when in zip(stages, at):
            def go(stage=stage):
                moves, before, after = build(src, refs)
                if stage > lo:
                    after(stage - 1, out)
                before(stage)
                start_all(moves[stage]())

            at_step(step, when, go)

    def tail(src, out, refs):
        build(src, refs)[2](hi, out)

    return Carry(in_shape, lo == 0, out_shape, scratch, head, tail)


def carry_rows(shape, start, count, when):
    def move(src, out, refs):
        return remote(src.at[pl.ds(start, count)], out, refs, 0, places()[3])

    def head(step, src, out, refs):
        at_step(step, when, lambda: move(src, out, refs).start())

    def tail(src, out, refs):
        move(src, out, refs).wait()

    return Carry(shape, True, (count,) + shape[1:], dma_sems(1), head, tail, True)


def carrier_call(body, ident, carries, travel, grid, in_specs, args, out_specs, out_shape, aliases, cost_estimate):
    n_in, n_out, n_c = len(in_specs), len(out_specs), len(carries)
    c_in = [pl.BlockSpec(memory_space=pl.ANY) if c.in_hbm else whole(c.in_shape) for c in carries]

    def kernel(*refs):
        ins, c_ins = refs[:n_in], refs[n_in:n_in + n_c]
        rest = refs[n_in + n_c:]
        outs, c_outs, scratch = rest[:n_out], rest[n_out:n_out + n_c], rest[n_out + n_c:]
        parts = []
        for c in carries:
            parts.append(scratch[:len(c.scratch)])
            scratch = scratch[len(c.scratch):]
        step = pl.program_id(0)

        @pl.when(step == 0)
        def _():
            _, _, _, at_core, at_x, at_y = places()
            meet((at_core, at_x, at_y))

        for c, src, out, refs_c in zip(carries, c_ins, c_outs, parts):
            c.head(step, src, out, refs_c)
        body(*ins, *outs)

        @pl.when(step == grid - 1)
        def _():
            for c, src, out, refs_c in zip(carries, c_ins, c_outs, parts):
                c.tail(src, out, refs_c)

    return pl.pallas_call(
        kernel,
        grid=(grid,),
        in_specs=in_specs + c_in,
        out_specs=out_specs + [pl.BlockSpec(memory_space=pl.ANY) if c.out_hbm else whole(c.out_shape) for c in carries],
        out_shape=out_shape + [jax.ShapeDtypeStruct(c.out_shape, F32) for c in carries],
        scratch_shapes=[shape for c in carries for shape in c.scratch],
        input_output_aliases=aliases,
        compiler_params=pltpu.CompilerParams(
            vmem_limit_bytes=VMEM_LIMIT, dimension_semantics=("arbitrary",), collective_id=ident,
            has_side_effects=True),
        cost_estimate=cost_estimate,
    )(*args, *travel)


def combine(mine, other):
    top_a, top_b = column(mine, MAX_LANE), column(other, MAX_LANE)
    top = jnp.maximum(top_a, top_b)
    fa, fb = jnp.exp2(top_a - top), jnp.exp2(top_b - top)
    inv = 1.0 / (column(mine, SUM_LANE) * fa + column(other, SUM_LANE) * fb)
    ax = mine * (fa * inv) + other * (fb * inv)
    lane = lax.broadcasted_iota(jnp.int32, ax.shape, 1)
    return jnp.where(lane < CH, ax, 0.0), top, inv


def mlp_a_kernel(axa_ref, axb_ref, z0_ref, wvo_ref, mg_ref, ms_ref, w1_ref, b1_ref, w2_ref, b2_ref, do_ref,
                 z1_ref, h_ref, slope_ref, z2_ref, full_ref, dw2_ref, act_ref):
    ax, _, _ = combine(axa_ref[0], axb_ref[0])
    z1 = z0_ref[:] + mm(ax[:, :CPAD].astype(BF16), wvo_ref[:])
    z1_ref[0] = z1
    h = layer_norm(z1, mg_ref[:], ms_ref[:]).astype(BF16)
    h_ref[0] = h
    d_out = do_ref[0]

    @pl.when(pl.program_id(0) == 0)
    def _():
        dw2_ref[:] = jnp.zeros_like(dw2_ref)

    n = h.shape[0] // 2
    for rows_of in (slice(0, n), slice(n, 2 * n)):
        pre = mm(h[rows_of], w1_ref[:]) + b1_ref[:]
        sq = pre * pre
        t = jnp.tanh(pre * (GELU_A + (GELU_A * GELU_B) * sq))
        half_t = 0.5 + 0.5 * t
        act = (pre * half_t).astype(BF16)
        slope_ref[0, rows_of] = half_t + (0.5 * pre) * (1.0 - t * t) * (GELU_A + (3.0 * GELU_A * GELU_B) * sq)
        act_ref[rows_of] = act
        z2 = z1_ref[0, rows_of] + mm(act, w2_ref[:]) + b2_ref[:]
        z2_ref[0, rows_of] = z2
        full_ref[0, rows_of] = z2
    dw2_ref[:] += mm(act_ref[:].T, d_out)


def mlp_a(axa, axb, z0, wvo, mg, ms, w1, b1, w2, b2, d_out):
    half, n, _ = axa.shape
    d = z0.shape[1]
    per = lambda c: lead((1, n, c))
    shifted = lead((1, n, d), lambda i: lax.axis_index('cp') * half + i)
    return pl.pallas_call(
        mlp_a_kernel,
        grid=(half,),
        in_specs=[per(AXW), per(AXW), once((n, d)), once((CPAD, d)), whole((1, d)), whole((1, d)),
                  once((d, d)), whole((1, d)), once((d, d)), whole((1, d)), shifted],
        out_specs=[per(d), per(d), per(d), per(d), shifted, whole((d, d))],
        out_shape=[
            jax.ShapeDtypeStruct((half, n, d), F32),
            jax.ShapeDtypeStruct((half, n, d), BF16),
            jax.ShapeDtypeStruct((half, n, d), F32),
            jax.ShapeDtypeStruct((half, n, d), F32),
            jax.ShapeDtypeStruct(d_out.shape, F32),
            jax.ShapeDtypeStruct((d, d), F32),
        ],
        scratch_shapes=[pltpu.VMEM((n, d), BF16)],
        compiler_params=params(),
        cost_estimate=cost(2 * half * n * d * (3 * d + 512), half * n * d * 18),
        name="mlp_a",
    )(axa, axb, z0, wvo, mg, ms, w1, b1, w2, b2, d_out)


def mlp_w_kernel(h_ref, slope_ref, do_ref, w2_ref, dpre_ref, dw1_ref, db1_ref):
    @pl.when(pl.program_id(0) == 0)
    def _():
        dw1_ref[:] = jnp.zeros_like(dw1_ref)
        db1_ref[:] = jnp.zeros_like(db1_ref)

    d_act = mm_nt(do_ref[0], w2_ref[:]).astype(BF16).astype(F32)
    d_pre = d_act * slope_ref[0]
    db1_ref[:] += jnp.sum(d_pre, axis=0, keepdims=True)
    d_pre_low = d_pre.astype(BF16)
    dpre_ref[0] = d_pre_low
    dw1_ref[:] += mm(h_ref[0].T, d_pre_low)


def mlp_w(h, slope, d_out, w2, carries, travel):
    half, n, d = h.shape
    per = lambda c: lead((1, n, c))
    return carrier_call(
        mlp_w_kernel, 5, carries, travel, half,
        [per(d), per(d), lead((1, n, d), lambda i: lax.axis_index('cp') * half + i), whole((d, d))],
        [h, slope, d_out, w2],
        [per(d), whole((d, d)), whole((1, d))],
        [jax.ShapeDtypeStruct((half, n, d), BF16), jax.ShapeDtypeStruct((d, d), F32), jax.ShapeDtypeStruct((1, d), F32)],
        {}, cost(2 * half * n * d * 2 * d, half * n * d * 10))


def mlp_b_kernel(axa_ref, axb_ref, z1_ref, dpre_ref, do_ref, wvo_ref, mg_ref, w1_ref, db1_ref, g_ref, acc_ref):
    ax, top, inv = combine(axa_ref[0], axb_ref[0])
    n, _ = z1_ref.shape[1:]
    z1 = z1_ref[0]
    d_hid = mm_nt(dpre_ref[0], w1_ref[:]).astype(BF16).astype(F32)
    centred = z1 - jnp.mean(z1, axis=1, keepdims=True)
    rstd = lax.rsqrt(jnp.mean(centred * centred, axis=1, keepdims=True) + LN_EPS)
    hat = centred * rstd
    d_hat = d_hid * mg_ref[:]
    mean_a = jnp.mean(d_hat, axis=1, keepdims=True)
    mean_b = jnp.mean(d_hat * hat, axis=1, keepdims=True)
    d_out = do_ref[0].astype(F32)
    d_mid = d_out + rstd * (d_hat - mean_a - hat * mean_b)
    d_mid_low = d_mid.astype(BF16)

    @pl.when(pl.program_id(0) == 0)
    def _():
        acc_ref[:] = jnp.zeros_like(acc_ref)
        acc_ref[VEC_ROW + 3:VEC_ROW + 4, :] = db1_ref[:]

    p = mm(ax[:, :CPAD].astype(BF16).T, d_mid_low)
    acc_ref[0:n, :] += d_mid
    acc_ref[n:n + CPAD, :] += p
    acc_ref[VEC_ROW:VEC_ROW + 1, :] += jnp.sum(d_hid * hat, axis=0, keepdims=True)
    acc_ref[VEC_ROW + 1:VEC_ROW + 2, :] += jnp.sum(d_hid, axis=0, keepdims=True)
    acc_ref[VEC_ROW + 2:VEC_ROW + 3, :] += jnp.sum(d_out, axis=0, keepdims=True)
    d_ax = jnp.concatenate([mm_nt(d_mid_low, wvo_ref[:]), jnp.zeros((n, AXW - CPAD), F32)], axis=1)
    delta = jnp.sum(d_ax * ax, axis=1, keepdims=True)
    lane = lax.broadcasted_iota(jnp.int32, d_ax.shape, 1)
    g_ref[0] = jnp.where(lane == SUM_LANE, delta, jnp.where(lane == MAX_LANE, top, jnp.where(lane == INV_LANE, inv, d_ax)))


def mlp_b(axa, axb, z1, dpre, d_out, wvo, mg, w1, db1, carries, travel):
    half, n, _ = axa.shape
    d = z1.shape[2]
    per = lambda c: lead((1, n, c))
    shifted = lead((1, n, d), lambda i: lax.axis_index('cp') * half + i)
    return carrier_call(
        mlp_b_kernel, 1, carries, travel, half,
        [per(AXW), per(AXW), per(d), per(d), shifted, once((CPAD, d)), whole((1, d)), once((d, d)), whole((1, d))],
        [axa, axb, z1, dpre, d_out, wvo, mg, w1, db1],
        [per(AXW), whole((ACC_ROWS, d))],
        [jax.ShapeDtypeStruct((half, n, AXW), F32), jax.ShapeDtypeStruct((ACC_ROWS, d), F32)],
        {}, cost(2 * half * n * d * (d + 800), half * n * d * 10))


def attn_bwd_body(g_ref, ax_ref, e_ref, xn_ref, qpt_ref, t_in_ref, dxn_ref, t_ref):
    g = g_ref[0]
    xn = xn_ref[0]
    e = e_ref[0]
    beta = jnp.exp2(column(ax_ref[0], MAX_LANE) - column(g, MAX_LANE)) * column(g, INV_LANE)
    lane = lax.broadcasted_iota(jnp.int32, g.shape, 1)
    scaled = g * beta
    d_low = jnp.where(lane < CH, scaled, 0.0)[:, :CPAD].astype(BF16)
    d_a = mm(d_low, xn)
    d_s = (e.astype(F32) * (d_a - column(scaled, SUM_LANE))).astype(BF16)

    @pl.when(pl.program_id(0) == 0)
    def _():
        t_ref[:] = t_in_ref[:]

    t_ref[:] += mm_nt(xn, d_s)
    dxn_ref[0] = (mm(qpt_ref[:], d_s) + mm(d_low.T, e)).astype(BF16)


def attn_bwd(own, g, ax, e, xn, qpt, t_in, dxn_in, ident, carries, travel):
    half, n, m = e.shape
    per = lambda c: lead((1, n, c))

    def at(i):
        core = lax.axis_index('cp')
        return (core if own else 1 - core) * half + i

    shifted = lead((1, CPAD, m), at)
    in_specs = [per(AXW), per(AXW), per(m), shifted, whole((CPAD, n)), whole((CPAD, n))]
    args = [g, ax, e, xn, qpt, t_in]
    aliases = {}
    if dxn_in is not None:
        in_specs.append(pl.BlockSpec(memory_space=pl.ANY))
        args.append(dxn_in)
        aliases = {6: 0}

    def body(*refs):
        attn_bwd_body(*refs[:6], *refs[-2:])

    return carrier_call(
        body, ident, carries, travel, half, in_specs, args,
        [shifted, whole((CPAD, n))],
        [jax.ShapeDtypeStruct(xn.shape, BF16), jax.ShapeDtypeStruct((CPAD, n), F32)],
        aliases, cost(8 * half * n * m * 512, half * n * m * 6))


def x_post_kernel(base_ref, gain_ref, x_ref, mean_ref, rstd_ref, dxn_ref, za_ref, zb_ref, wa_ref, wb_ref, full_in_ref, dx_ref, sums_ref, full_ref, w_ref,
                  rows_ref, dg_ref, ds_ref):
    nb, lanes = x_ref.shape[1:]
    pitch = CPAD + ROW_GAP
    late = pl.program_id(0) >= pl.num_programs(0) // 2
    mine = late == (base_ref[0] == 1)

    @pl.when(late)
    def _():
        full_ref[0] = zb_ref[0]

    @pl.when(jnp.logical_not(late))
    def _():
        full_ref[0] = za_ref[0]

    @pl.when(mine)
    def _():
        w_ref[:] = wa_ref[:]

    @pl.when(jnp.logical_not(mine))
    def _():
        w_ref[:] = wb_ref[:]

    for b in range(nb):
        rows_ref[b * pitch:b * pitch + CPAD, :] = dxn_ref[b].astype(F32)
    zero = jnp.zeros((nb, lanes), F32)
    mean = mean_ref[:]
    rstd = rstd_ref[:]

    @pl.when(pl.program_id(0) == 0)
    def _():
        dg_ref[:] = jnp.zeros_like(dg_ref)
        ds_ref[:] = jnp.zeros_like(ds_ref)

    def gather(c, acc):
        da, db = acc
        hat = (x_ref[c].astype(F32) - mean) * rstd
        dxn = rows_ref[pl.ds(c, nb, stride=pitch), :]
        dh = dxn * gain_ref[c]
        prod = dxn * hat
        dg_ref[c] += prod[:8] + prod[8:]
        ds_ref[c] += dxn[:8] + dxn[8:]
        return da + dh, db + dh * hat

    da, db = lax.fori_loop(0, CH, gather, (zero, zero), unroll=9)
    mean_a = da * (1.0 / CH)
    mean_b = db * (1.0 / CH)

    def put(c, carry):
        hat = (x_ref[c].astype(F32) - mean) * rstd
        dxn = rows_ref[pl.ds(c, nb, stride=pitch), :]
        dx_ref[c] = (rstd * (dxn * gain_ref[c] - mean_a - hat * mean_b)).astype(BF16)
        return carry

    lax.fori_loop(0, CH, put, 0, unroll=9)

    @pl.when(pl.program_id(0) == pl.num_programs(0) - 1)
    def _():
        for k, ref in enumerate((dg_ref, ds_ref)):
            part = jnp.concatenate([jnp.sum(ref[:], axis=1), jnp.zeros((AXW - CH, lanes), F32)], axis=0)
            sums_ref[k:k + 1, :] = jnp.sum(part.T, axis=0, keepdims=True)


def x_post(core, x_gain, x_cm, mean, rstd, dxn, za, zb, full, w_own, w_got):
    _, nb, m = x_cm.shape
    half, n, d = 2 * za.shape[0], *za.shape[1:]
    lanes = m // half
    slab = 2 * w_own.shape[0] // half
    chan = trail((CH, nb, lanes))
    stat = trail((nb, lanes))

    def piece(side):
        last = half // 2 - 1
        return pl.BlockSpec((slab, d), lambda i, core: (
            jnp.clip(i - (core[0] if side else 1 - core[0]) * (half // 2), 0, last), 0))

    return pl.pallas_call(
        x_post_kernel,
        grid_spec=pltpu.PrefetchScalarGridSpec(
            num_scalar_prefetch=1,
            grid=(half,),
            in_specs=[
                pl.BlockSpec(memory_space=pltpu.SMEM),
                chan, stat, stat,
                trail((nb, CPAD, lanes)),
                lead((1, n, d), lambda i: jnp.minimum(i, half // 2 - 1)),
                lead((1, n, d), lambda i: jnp.maximum(i - half // 2, 0)),
                piece(True), piece(False),
                pl.BlockSpec(memory_space=pl.ANY),
            ],
            out_specs=[chan, whole((2, AXW)), pl.BlockSpec((1, n, d), lambda i, core: ((1 - core[0]) * half + i, 0, 0)),
                       lead((slab, d))],
            scratch_shapes=[pltpu.VMEM(((CPAD + ROW_GAP) * nb, lanes), F32),
                            pltpu.VMEM((CH, 8, lanes), F32), pltpu.VMEM((CH, 8, lanes), F32)],
        ),
        out_shape=[
            jax.ShapeDtypeStruct(x_cm.shape, BF16),
            jax.ShapeDtypeStruct((2, AXW), F32),
            jax.ShapeDtypeStruct(full.shape, F32),
            jax.ShapeDtypeStruct((2 * w_own.shape[0], d), F32),
        ],
        input_output_aliases={10: 2},
        compiler_params=params(),
        cost_estimate=cost(6e9, 6 * nb * CH * m + 8 * half * n * d),
        name="x_post",
    )(core, x_gain, x_cm, mean, rstd, dxn, za, zb, w_own, w_got, full)


def finish_kernel(devices, x_ref, ta_ref, tb_ref, tc_ref, td_ref, own_ref, gx_ref, gy_ref, o_ref, t_ref, acc_ref,
                  got_ref, t_all, acc_all, send_sem, recv_sem):
    dp, cp = devices
    my_dp, my_cp = lax.axis_index('dp'), lax.axis_index('cp')
    core, x, y, at_core, _, _ = places()
    peers = [(i, j) for i in range(dp) for j in range(cp)][1:]
    ids = [(lax.rem(my_dp + i, dp), lax.rem(my_cp + j, cp)) for i, j in peers]
    meet(ids)
    copies = [remote(x_ref, got_ref.at[k], (send_sem, recv_sem), k, dev) for k, dev in enumerate(ids)]
    start_all(copies)
    th, ah = ta_ref.shape[0], 4 * own_ref.shape[1]
    eighth = own_ref.shape[1]
    base = core * ah
    t_all[pl.ds(pl.multiple_of(core * th, 8), th), :] = (ta_ref[:] + tb_ref[:]) + (tc_ref[:] + td_ref[:])
    t_copy = remote(rows(t_all, core * th, th), rows(t_all, core * th, th), (send_sem, recv_sem), len(ids), at_core)
    for start, ref in ((x * eighth, own_ref.at[0]), ((1 - x) * eighth, gx_ref),
                       ((2 + y) * eighth, own_ref.at[1]), ((3 - y) * eighth, gy_ref)):
        acc_all[pl.ds(pl.multiple_of(base + start, 8), eighth), :] = ref[:]
    t_copy.start()
    acc_copy = remote(rows(acc_all, base, ah), rows(acc_all, base, ah), (send_sem, recv_sem), len(ids) + 1, at_core)
    acc_copy.start()
    wait_all(copies)
    o_ref[:] = x_ref[:] + jnp.sum(got_ref[:], axis=0)
    t_copy.wait()
    t_ref[:] = t_all[:]
    acc_copy.wait()
    acc_ref[:] = acc_all[:]


def finish(mesh, x, t_parts, own, got_x, got_y):
    count = mesh.size - 1
    t_shape = (2 * t_parts[0].shape[0], t_parts[0].shape[1])
    acc_shape = (8 * own.shape[1], own.shape[2])
    vmem = pl.BlockSpec(memory_space=pltpu.VMEM)
    return pl.pallas_call(
        functools.partial(finish_kernel, (mesh.shape['dp'], mesh.shape['cp'])),
        in_specs=[vmem] * 8,
        out_specs=[vmem] * 3,
        out_shape=[jax.ShapeDtypeStruct(shape, F32) for shape in (x.shape, t_shape, acc_shape)],
        scratch_shapes=[pltpu.VMEM((count,) + x.shape, F32), pltpu.VMEM(t_shape, F32), pltpu.VMEM(acc_shape, F32)]
        + dma_sems(count + 2),
        compiler_params=pltpu.CompilerParams(vmem_limit_bytes=VMEM_LIMIT, collective_id=0, has_side_effects=True),
        name="finish",
    )(x, *t_parts, own, got_x, got_y)


def prologue_kernel(scale, z0_ref, zg_ref, zs_ref, wq_ref, wk_in_ref, wv_in_ref, wo_ref,
                    zn_ref, q_ref, qp_ref, qpt_ref, wvo_ref, wk_ref, wv_ref):
    for src, dst in ((wk_in_ref, wk_ref), (wv_in_ref, wv_ref)):
        dst[256:, :] = jnp.zeros((CPAD - 256, src.shape[1]), BF16)
        dst[:CH, :] = src[:]
    zn = layer_norm(z0_ref[:], zg_ref[:], zs_ref[:]).astype(BF16)
    zn_ref[:] = zn
    q = mm(zn, wq_ref[:]).astype(BF16)
    q_ref[:] = q
    wk = wk_ref[:]
    qp_ref[:] = (mm_nt(q, wk) * (scale * LOG2E)).astype(BF16)
    qpt_ref[:] = (mm_nt(wk, q) * scale).astype(BF16)
    wvo_ref[:] = mm(wv_ref[:], wo_ref[:]).astype(BF16)


def prologue(scale, z0, zg, zs, wq, wk, wv, wo):
    n, d = z0.shape
    vmem = pl.BlockSpec(memory_space=pltpu.VMEM)
    return pl.pallas_call(
        functools.partial(prologue_kernel, scale),
        in_specs=[vmem] * 7,
        out_specs=[vmem] * 7,
        out_shape=[jax.ShapeDtypeStruct(shape, BF16)
                   for shape in ((n, d), (n, d), (n, CPAD), (CPAD, n), (CPAD, d), (CPAD, d), (CPAD, d))],
        compiler_params=pltpu.CompilerParams(vmem_limit_bytes=VMEM_LIMIT),
        cost_estimate=cost(3e9, 12e6),
        name="prologue",
    )(z0, zg, zs, wq, wk, wv, wo)


def final_kernel(scale, t_ref, acc_ref, z0_ref, zg_ref, zn_ref, q_ref, wq_ref, wk_ref, wv_ref, wo_ref,
                 dlat_ref, dzg_ref, dzs_ref, dwq_ref, dwk_ref, dwv_ref, dwo_ref):
    n = z0_ref.shape[0]
    p_low = acc_ref[n:n + CPAD, :].astype(BF16)
    dwo_ref[:] = mm(wv_ref[:].T, p_low)
    dwv_ref[:] = mm_nt(p_low, wo_ref[:])[:CH]
    t_low = (t_ref[:] * scale).astype(BF16)
    dwk_ref[:] = mm(t_low, q_ref[:])[:CH]
    d_q = mm(t_low.T, wk_ref[:]).astype(BF16)
    dwq_ref[:] = mm(zn_ref[:].T, d_q)
    d_zn = mm_nt(d_q, wq_ref[:])
    z0 = z0_ref[:]
    centred = z0 - jnp.mean(z0, axis=1, keepdims=True)
    rstd = lax.rsqrt(jnp.mean(centred * centred, axis=1, keepdims=True) + LN_EPS)
    hat = centred * rstd
    dzg_ref[:] = jnp.sum(d_zn * hat, axis=0, keepdims=True)
    dzs_ref[:] = jnp.sum(d_zn, axis=0, keepdims=True)
    d_hat = d_zn * zg_ref[:]
    mean_a = jnp.mean(d_hat, axis=1, keepdims=True)
    mean_b = jnp.mean(d_hat * hat, axis=1, keepdims=True)
    dlat_ref[:] = acc_ref[:n, :] + rstd * (d_hat - mean_a - hat * mean_b)


def final(scale, t, acc, z0, zg, zn, q, wq, wk, wv, wo):
    n, d = z0.shape
    vmem = pl.BlockSpec(memory_space=pltpu.VMEM)
    shapes = ((n, d), (1, d), (1, d), (d, d), (CH, d), (CH, d), (d, d))
    return pl.pallas_call(
        functools.partial(final_kernel, scale),
        in_specs=[vmem] * 10,
        out_specs=[vmem] * 7,
        out_shape=[jax.ShapeDtypeStruct(shape, F32) for shape in shapes],
        compiler_params=pltpu.CompilerParams(vmem_limit_bytes=VMEM_LIMIT),
        cost_estimate=cost(4e9, 25e6),
        name="final",
    )(t, acc, z0, zg, zn, q, wq, wk, wv, wo)


def solution(mesh):
    x_spec, row_spec = P('dp', 'cp'), P('dp')
    vec_spec = mat_spec = P()
    in_specs = (x_spec, mat_spec, vec_spec, vec_spec, vec_spec, vec_spec, mat_spec, mat_spec, mat_spec, mat_spec,
                vec_spec, vec_spec, mat_spec, vec_spec, mat_spec, vec_spec, row_spec)
    out_specs = (row_spec, x_spec, mat_spec, vec_spec, vec_spec, vec_spec, vec_spec, mat_spec, mat_spec, mat_spec, mat_spec,
                 vec_spec, vec_spec, mat_spec, vec_spec, mat_spec, vec_spec)
    swap = [(0, 1), (1, 0)]

    def step(inputs, latents, x_gain, x_shift, z_gain, z_shift, w_query, w_key, w_value, w_out, m_gain, m_shift, w_up, b_up, w_down, b_down, d_out):
        qk_scale = w_query.shape[1] ** -0.5
        n, d = latents.shape
        half = inputs.shape[0] // 2
        core = lax.axis_index('cp')
        as_ints = lambda *vals: jnp.stack([v.astype(jnp.int32) for v in vals])
        mine = as_ints(core * half, core * (d // 2))
        other = as_ints((1 - core) * half, (1 - core) * (d // 2))
        row = lambda vec: vec.reshape(1, -1)

        x_cm = jnp.transpose(inputs, (2, 0, 1))
        xn, x_mean, x_rstd = x_prep(x_cm, x_gain, x_shift)

        z_norm, queries, qp, qpt, wvo, wk_pad, wv_pad = prologue(
            qk_scale, latents, row(z_gain), row(z_shift), w_query, w_key, w_value, w_out)

        e_other, ax_other = attn_fwd(other, qp, xn, half)
        ax_got = lax.ppermute(ax_other, 'cp', swap)
        e_mine, ax_mine = attn_fwd(mine, qp, xn, half)

        flip = lambda bit: [(k, k ^ bit) for k in range(4)]
        z1, hid, slope, z2, full, dw2 = mlp_a(
            ax_mine, ax_got, latents, wvo, row(m_gain), row(m_shift), w_up, row(b_up), w_down, row(b_down), d_out)
        dpre, dw1, db1, w2_pieces = mlp_w(
            hid, slope, d_out, w_down, [carry(d, d, (0, 1, 2), (0, 2, 6))], [dw2])
        g_mine, acc, w2_half, w1_eighths, za_got = mlp_b(
            ax_mine, ax_got, z1, dpre, d_out, wvo, row(m_gain), w_up, db1,
            [carry(d, d, (3, 4), (0, 2)), carry(d, d, (0, 1), (0, 2)), carry_rows(z2.shape, 0, half // 2, 2)],
            [w2_pieces, dw1, z2])
        g_got = lax.ppermute(g_mine, 'cp', swap)
        dxn, t_part, w1_eighths, acc_half = attn_bwd(
            True, g_mine, ax_mine, e_mine, xn, qpt, jnp.zeros((CPAD, n), F32), None, 3,
            [carry(d, d, (2, 3), (0, 3)), carry(ACC_ROWS, d, (0,), (0,))], [w1_eighths, acc])
        w2_half, dxn = lax.optimization_barrier((w2_half, dxn))
        w2_got = lax.ppermute(w2_half, 'cp', swap)
        dxn, t_part, acc_eighths, zb_got = attn_bwd(
            False, g_got, ax_other, e_other, xn, qpt, t_part, dxn, 4,
            [carry(ACC_ROWS, d, (1, 2, 3), (0, 5, 7)), carry_rows(z2.shape, half // 2, half // 2, 0)],
            [acc_half, z2])
        w1_eighths, dxn = lax.optimization_barrier((w1_eighths, dxn))

        def halves(own):
            got_x = lax.ppermute(own[0], 'dp', flip(1))
            got_y = lax.ppermute(own[1], 'dp', flip(2))
            return got_x, got_y

        w1_x, w1_y = halves(w1_eighths)
        acc_x, acc_y = halves(acc_eighths)

        t_mine = lax.dynamic_slice_in_dim(t_part, core * (CPAD // 2), CPAD // 2, 0)
        t_send = lax.dynamic_slice_in_dim(t_part, (1 - core) * (CPAD // 2), CPAD // 2, 0)
        t_mine = t_mine + lax.ppermute(t_send, 'cp', swap)
        t_parts = [t_mine]
        for bit in (1, 2, 3):
            t_parts.append(lax.ppermute(t_mine, 'dp', [(k, k ^ bit) for k in range(4)]))
        dx_cm, sums, z_out, d_w_down = x_post(
            core.astype(jnp.int32).reshape(1), x_gain, x_cm, x_mean, x_rstd, dxn, za_got, zb_got, full, w2_half, w2_got)
        sums, t_sum, acc = finish(mesh, sums, t_parts, acc_eighths, acc_x, acc_y)
        d_x_gain, d_x_shift = sums[0, :CH], sums[1, :CH]
        order = lambda bit, own, got: jnp.where(
            bit == 0, jnp.concatenate([own, got], 0), jnp.concatenate([got, own], 0))
        chip = lax.axis_index('dp')
        w1_half = jnp.concatenate([
            order(lax.rem(chip, 2), w1_eighths[0], w1_x), order(chip // 2, w1_eighths[1], w1_y)], 0)
        w1_got = lax.ppermute(w1_half, 'cp', swap)
        d_w_up = order(core, w1_half, w1_got)

        d_m_gain, d_m_shift, d_b_down, d_b_up = (acc[VEC_ROW + k] for k in range(4))
        d_lat, d_z_gain, d_z_shift, d_w_query, d_w_key, d_w_value, d_w_out = final(
            qk_scale, t_sum, acc, latents, row(z_gain), z_norm, queries, w_query, wk_pad, wv_pad, w_out)
        return (z_out, jnp.transpose(dx_cm, (1, 2, 0)), d_lat, d_x_gain, d_x_shift, d_z_gain[0], d_z_shift[0],
                d_w_query, d_w_key, d_w_value, d_w_out, d_m_gain, d_m_shift, d_w_up, d_b_up, d_w_down, d_b_down)

    return jax.shard_map(step, mesh=mesh, in_specs=in_specs, out_specs=out_specs, check_vma=False)
```

```python
import functools
import math

import jax
import jax.numpy as jnp
from jax import lax
from jax.experimental import pallas as pl
from jax.experimental.pallas import tpu as pltpu
from jax.sharding import PartitionSpec as P


LN_EPS = 1e-5
F32 = jnp.float32
BF16 = jnp.bfloat16
CH = 261
CPAD = 272
AXW = 384
ROW_GAP = 8
ACC_ROWS = 896
VEC_ROW = 784
SUM_LANE = 261
MAX_LANE = 262
INV_LANE = 263
LOG2E = math.log2(math.e)
GELU_A = math.sqrt(2.0 / math.pi)
GELU_B = 0.044715
VMEM_LIMIT = 63 * 1024 * 1024


def layer_norm(tensor, ln_gain, ln_shift):
    row_mean = jnp.mean(tensor, axis=-1, keepdims=True)
    centred = tensor - row_mean
    variance = jnp.mean(centred * centred, axis=-1, keepdims=True)
    return centred * lax.rsqrt(variance + LN_EPS) * ln_gain + ln_shift


def mm(lhs, rhs):
    return lax.dot_general(lhs, rhs, (((1,), (0,)), ((), ())), preferred_element_type=F32)


def mm_nt(lhs, rhs):
    return lax.dot_general(lhs, rhs, (((1,), (1,)), ((), ())), preferred_element_type=F32)


def params(semantics=1):
    return pltpu.CompilerParams(
        vmem_limit_bytes=VMEM_LIMIT, dimension_semantics=("arbitrary",) * semantics)


def whole(shape, **kw):
    return pl.BlockSpec(shape, lambda *_: (0,) * len(shape), **kw)


def once(shape):
    return whole(shape, pipeline_mode=pl.Buffered(1))


def lead(shape, index=lambda i: i):
    return pl.BlockSpec(shape, lambda i, *_: (index(i),) + (0,) * (len(shape) - 1))


def trail(shape):
    return pl.BlockSpec(shape, lambda i, *_: (0,) * (len(shape) - 1) + (i,))


def row_mean(array):
    return jnp.mean(array, axis=1, keepdims=True)


def row_sum(array):
    return jnp.sum(array, axis=1, keepdims=True)


def col_sum(array):
    return jnp.sum(array, axis=0, keepdims=True)


def column(array, lane):
    return array[:, lane:lane + 1]


def cost(flops, nbytes):
    return pl.CostEstimate(flops=int(flops), bytes_accessed=int(nbytes), transcendentals=0)


def over_channels(term, zero):
    third = CH // 3
    parts = lax.fori_loop(
        0, third, lambda c, acc: tuple(a + term(c + k * third) for k, a in enumerate(acc)), (zero,) * 3, unroll=29)
    return sum(parts[1:], parts[0]) * (1.0 / CH)


def x_prep_kernel(gain_ref, shift_ref, x_ref, xn_ref, mean_ref, rstd_ref, *rows_refs):
    nb, lanes = x_ref.shape[1:]
    pitch = nb + ROW_GAP
    width = lanes // len(rows_refs)
    zero = jnp.zeros((nb, lanes), F32)
    mean = over_channels(lambda c: x_ref[c].astype(F32), zero)

    def square(c):
        d = x_ref[c].astype(F32) - mean
        return d * d

    rstd = lax.rsqrt(over_channels(square, zero) + LN_EPS)
    mean_ref[:] = mean
    rstd_ref[:] = rstd

    def put(c, carry):
        xn = (x_ref[c].astype(F32) - mean) * rstd * gain_ref[c] + shift_ref[c]
        for k, ref in enumerate(rows_refs):
            ref[pl.ds(pl.multiple_of(c * pitch, ROW_GAP), nb), :] = xn[:, k * width:(k + 1) * width]
        return carry

    lax.fori_loop(0, CH, put, 0, unroll=9)
    for k, ref in enumerate(rows_refs):
        ref[CH * pitch:CPAD * pitch, :] = jnp.zeros(((CPAD - CH) * pitch, width), F32)
        for b in range(nb):
            xn_ref[b, :, k * width:(k + 1) * width] = ref[pl.ds(b, CPAD, stride=pitch), :].astype(BF16)


def x_prep(x_cm, x_gain, x_shift):
    _, nb, m = x_cm.shape
    lanes = 256
    return pl.pallas_call(
        x_prep_kernel,
        grid=(m // lanes,),
        in_specs=[
            pl.BlockSpec(memory_space=pltpu.SMEM),
            pl.BlockSpec(memory_space=pltpu.SMEM),
            trail((CH, nb, lanes)),
        ],
        out_specs=[trail((nb, CPAD, lanes)), trail((nb, lanes)), trail((nb, lanes))],
        out_shape=[
            jax.ShapeDtypeStruct((nb, CPAD, m), BF16),
            jax.ShapeDtypeStruct((nb, m), F32),
            jax.ShapeDtypeStruct((nb, m), F32),
        ],
        scratch_shapes=[pltpu.VMEM((CPAD * (nb + ROW_GAP), 128), F32)] * 2,
        compiler_params=params(),
        cost_estimate=cost(3e9, 4 * nb * CH * m),
        name="x_prep",
    )(x_gain, x_shift, x_cm)


def attn_fwd_kernel(base_ref, qp_ref, xn_ref, e_ref, ax_ref):
    xn = xn_ref[0]
    n = qp_ref.shape[0]
    spans = [slice(k * (n // 2), (k + 1) * (n // 2)) for k in range(2)]
    logits = [mm(qp_ref[span, :], xn) for span in spans]
    for span, s in zip(spans, logits):
        top = jnp.max(s, axis=1, keepdims=True)
        e = jnp.exp2(s - top)
        total = row_sum(e)
        e_low = e.astype(BF16)
        e_ref[0, span, :] = e_low
        ax = jnp.concatenate([mm_nt(e_low, xn), jnp.zeros((e.shape[0], AXW - CPAD), F32)], axis=1)
        lane = lax.broadcasted_iota(jnp.int32, ax.shape, 1)
        ax_ref[0, span, :] = jnp.where(lane == SUM_LANE, total, jnp.where(lane == MAX_LANE, top, ax))


def attn_fwd(base, qp, xn, half):
    n = qp.shape[0]
    m = xn.shape[2]
    return pl.pallas_call(
        attn_fwd_kernel,
        grid_spec=pltpu.PrefetchScalarGridSpec(
            num_scalar_prefetch=1,
            grid=(half,),
            in_specs=[
                whole((n, CPAD)),
                pl.BlockSpec((1, CPAD, m), lambda i, base: (base[0] + i, 0, 0)),
            ],
            out_specs=[
                lead((1, n, m)),
                lead((1, n, AXW)),
            ],
        ),
        out_shape=[
            jax.ShapeDtypeStruct((half, n, m), BF16),
            jax.ShapeDtypeStruct((half, n, AXW), F32),
        ],
        compiler_params=params(),
        cost_estimate=cost(4 * half * n * m * 512, half * n * m * 3),
        name="attn_fwd",
    )(base, qp, xn)


def places():
    core, chip = lax.axis_index('cp'), lax.axis_index('dp')
    x, y = lax.rem(chip, 2), chip // 2
    at_x = (y * 2 + (1 - x), core)
    at_y = ((1 - y) * 2 + x, core)
    return core, x, y, (chip, 1 - core), at_x, at_y


def meet(devices):
    barrier = pltpu.get_barrier_semaphore()
    for dev in devices:
        pl.semaphore_signal(barrier, inc=1, device_id=dev, device_id_type=pl.DeviceIdType.MESH)
    pl.semaphore_wait(barrier, len(devices))


def remote(src, dst, sems, k, dev):
    return pltpu.make_async_remote_copy(
        src_ref=src, dst_ref=dst, send_sem=sems[0].at[k], recv_sem=sems[1].at[k],
        device_id=dev, device_id_type=pl.DeviceIdType.MESH)


def rows(ref, start, size):
    return ref.at[pl.ds(pl.multiple_of(start, 8), size)]


def take(ref, start, size):
    return ref[pl.ds(pl.multiple_of(start, 8), size), :]


def at_step(step, when, todo):
    pl.when(step == when)(todo)


def dma_sems(count):
    return [pltpu.SemaphoreType.DMA((count,)), pltpu.SemaphoreType.DMA((count,))]


class Carry:
    def __init__(self, in_shape, in_hbm, out_shapes, scratch, head, tail, out_hbm=False):
        self.in_shape, self.in_hbm, self.out_shapes, self.scratch = in_shape, in_hbm, out_shapes, scratch
        self.out_hbm = out_hbm
        self.head, self.tail = head, tail


def start_all(copies):
    for copy in copies:
        copy.start()


def wait_all(copies):
    for copy in copies:
        copy.wait()


class Plan:
    def __init__(self, total):
        self.half, self.quarter, self.eighth, self.part = (total // k for k in (2, 4, 8, 16))
        self.core, self.x, self.y, self.at_core, self.at_x, self.at_y = places()
        self.spot = (self.x * self.eighth, self.quarter + self.y * self.eighth)
        self.away = ((1 - self.x) * self.eighth, self.quarter + (1 - self.y) * self.eighth)
        self.fine = (self.y * self.part, self.x * self.part)
        self.fine_away = ((1 - self.y) * self.part, (1 - self.x) * self.part)
        self.first, self.second = (self.at_x, self.at_y), (self.at_y, self.at_x)


def carry(total, width, stages, at):
    half, _, eighth, part = (total // k for k in (2, 4, 8, 16))
    lo, hi = stages[0], stages[-1]
    in_shape = {0: (total, width), 1: (half, width), 2: (2, eighth, width), 3: (2, part, width)}[lo]
    out_shape = {0: (half, width), 1: (2, eighth, width), 2: (2, part, width), 3: (eighth, width), 4: (half, width)}[hi]
    shapes = {}
    if 0 in stages:
        shapes.update(half=(half, width), rx0=(half, width))
    if 1 in stages:
        shapes.update(rx1=(2, eighth, width))
    if 2 in stages:
        shapes.update(rx2=(2, part, width))
    if 1 in stages and 2 in stages:
        shapes.update(mid=(2, eighth, width))
    if 2 in stages and 3 in stages:
        shapes.update(fin=(2, part, width))
    if 3 in stages:
        shapes.update(buf=(2, eighth, width))
    if 4 in stages:
        shapes.update(full=(half, width))
    names = list(shapes)
    count = 2 * len(stages)
    scratch = [pltpu.VMEM(shape, F32) for shape in shapes.values()] + [pltpu.SemaphoreType.DMA((1,))] + dma_sems(count)

    def build(src, refs):
        r = dict(zip(names, refs))
        local, sems = refs[-3], (refs[-2], refs[-1])
        p = Plan(total)
        slot = lambda stage, k: 2 * (stage - lo) + k
        two = (0, 1)
        moves = {}
        if 0 in stages:
            moves[0] = lambda: [pltpu.make_async_copy(rows(src, p.core * half, half), r['half'], local.at[0]),
                                remote(rows(src, (1 - p.core) * half, half), r['rx0'], sems, slot(0, 0), p.at_core)]
        if 1 in stages:
            pair = r.get('half', src)
            moves[1] = lambda: [remote(rows(pair, p.away[k], eighth), r['rx1'].at[k], sems, slot(1, k), p.first[k])
                                for k in two]
        if 2 in stages:
            mid = r.get('mid', src)
            moves[2] = lambda: [remote(rows(mid.at[k], p.fine_away[k], part), r['rx2'].at[k], sems, slot(2, k), p.second[k])
                                for k in two]
        if 3 in stages:
            fin = r.get('fin', src)
            moves[3] = lambda: [remote(fin.at[k], rows(r['buf'].at[k], p.fine[k], part), sems, slot(3, k), p.second[k])
                                for k in two]
        if 4 in stages:
            moves[4] = lambda: [remote(r['buf'].at[k], rows(r['full'], p.spot[k], eighth), sems, slot(4, k), p.first[k])
                                for k in two]

        def before(stage):
            if stage == 3:
                for k in two:
                    r['buf'][k, pl.ds(pl.multiple_of(p.fine[k], 8), part), :] = fin[k]

        def after(stage, out):
            wait_all(moves[stage]())
            if stage == 0:
                r['half'][:] += r['rx0'][:]
                if hi == 0:
                    out[:] = r['half'][:]
            elif stage == 1:
                dst = out if hi == 1 else r['mid']
                for k in two:
                    dst[k] = take(pair, p.spot[k], eighth) + r['rx1'][k]
            elif stage == 2:
                dst = out if hi == 2 else r['fin']
                for k in two:
                    dst[k] = take(mid.at[k], p.fine[k], part) + r['rx2'][k]
            elif stage == 3 and hi == 3:
                for k in two:
                    out[k][:] = r['buf'][k]
            elif stage == 4:
                for k in two:
                    r['full'][pl.ds(pl.multiple_of(p.spot[k], 8), eighth), :] = r['buf'][k]
                out[:] = r['full'][:]

        return moves, before, after

    def head(step, src, outs, refs):
        out = outs if hi == 3 else outs[0]
        for stage, when in zip(stages, at):
            def go(stage=stage):
                moves, before, after = build(src, refs)
                if stage > lo:
                    after(stage - 1, out)
                before(stage)
                start_all(moves[stage]())

            at_step(step, when, go)

    def tail(src, outs, refs):
        build(src, refs)[2](hi, outs if hi == 3 else outs[0])

    return Carry(in_shape, lo == 0, [out_shape] * (2 if hi == 3 else 1), scratch, head, tail)


def carry_rows(shape, half, start, count, when):
    def move(src, outs, refs):
        core, _, _, at_core, _, _ = places()
        return remote(src.at[pl.ds(core * half + start, count)], outs[0], refs, 0, at_core)

    def head(step, src, outs, refs):
        at_step(step, when, lambda: move(src, outs, refs).start())

    def tail(src, outs, refs):
        move(src, outs, refs).wait()

    return Carry(shape, True, [(count,) + shape[1:]], dma_sems(1), head, tail, True)


def carrier_call(body, ident, carries, travel, grid, in_specs, args, out_specs, out_shape, aliases, cost_estimate):
    n_in, n_out, n_c = len(in_specs), len(out_specs), len(carries)
    c_in = [pl.BlockSpec(memory_space=pl.ANY) if c.in_hbm else whole(c.in_shape) for c in carries]

    def kernel(*refs):
        ins, c_ins = refs[:n_in], refs[n_in:n_in + n_c]
        rest = refs[n_in + n_c:]
        outs, scratch = rest[:n_out], rest[n_out + sum(len(c.out_shapes) for c in carries):]
        rest = rest[n_out:]
        c_outs, parts = [], []
        for c in carries:
            c_outs.append(rest[:len(c.out_shapes)])
            rest = rest[len(c.out_shapes):]
            parts.append(scratch[:len(c.scratch)])
            scratch = scratch[len(c.scratch):]
        step = pl.program_id(0)

        @pl.when(step == 0)
        def _():
            _, _, _, at_core, at_x, at_y = places()
            meet((at_core, at_x, at_y))

        for c, src, out, refs_c in zip(carries, c_ins, c_outs, parts):
            c.head(step, src, out, refs_c)
        body(*ins, *outs)

        @pl.when(step == grid - 1)
        def _():
            for c, src, out, refs_c in zip(carries, c_ins, c_outs, parts):
                c.tail(src, out, refs_c)

    return pl.pallas_call(
        kernel,
        grid=(grid,),
        in_specs=in_specs + c_in,
        out_specs=out_specs + [pl.BlockSpec(memory_space=pl.ANY) if c.out_hbm else whole(shape)
                               for c in carries for shape in c.out_shapes],
        out_shape=out_shape + [jax.ShapeDtypeStruct(shape, F32) for c in carries for shape in c.out_shapes],
        scratch_shapes=[shape for c in carries for shape in c.scratch],
        input_output_aliases=aliases,
        compiler_params=pltpu.CompilerParams(
            vmem_limit_bytes=VMEM_LIMIT, dimension_semantics=("arbitrary",), collective_id=ident,
            has_side_effects=True),
        cost_estimate=cost_estimate,
    )(*args, *travel)


def combine(mine, other):
    top_a, top_b = column(mine, MAX_LANE), column(other, MAX_LANE)
    top = jnp.maximum(top_a, top_b)
    fa, fb = jnp.exp2(top_a - top), jnp.exp2(top_b - top)
    inv = 1.0 / (column(mine, SUM_LANE) * fa + column(other, SUM_LANE) * fb)
    ax = mine * (fa * inv) + other * (fb * inv)
    lane = lax.broadcasted_iota(jnp.int32, ax.shape, 1)
    return jnp.where(lane < CH, ax, 0.0), top, inv


def mlp_a_kernel(axa_ref, axb_ref, z0_ref, wvo_ref, mg_ref, ms_ref, w1_ref, b1_ref, w2_ref, b2_ref, do_ref,
                 z1_ref, h_ref, slope_ref, full_ref, dw2_ref, act_ref):
    count, n, width = z1_ref.shape
    step = 512
    flat = lambda ref, cols: ref[:, :, cols].reshape(count * n, step)

    @pl.when(pl.program_id(0) == 0)
    def _():
        dw2_ref[:] = jnp.zeros_like(dw2_ref)

    for b in range(count):
        ax, _, _ = combine(axa_ref[b], axb_ref[b])
        z1 = z0_ref[:] + mm(ax[:, :CPAD].astype(BF16), wvo_ref[:])
        z1_ref[b] = z1
        h_ref[b] = layer_norm(z1, mg_ref[:], ms_ref[:]).astype(BF16)
    h = h_ref[:].reshape(count * n, width)
    spans = [slice(lo, lo + step) for lo in range(0, width, step)]
    for cols in spans:
        pre = mm(h, w1_ref[:, cols]) + b1_ref[:, cols]
        sq = pre * pre
        t = jnp.tanh(pre * (GELU_A + (GELU_A * GELU_B) * sq))
        half_t = 0.5 + 0.5 * t
        act_ref[:, cols] = (pre * half_t).astype(BF16)
        slope = half_t + (0.5 * pre) * (1.0 - t * t) * (GELU_A + (3.0 * GELU_A * GELU_B) * sq)
        slope_ref[:, :, cols] = slope.reshape(count, n, step)
    act = act_ref[:]
    for cols in spans:
        z2 = flat(z1_ref, cols) + mm(act, w2_ref[:, cols]) + b2_ref[:, cols]
        full_ref[:, :, cols] = z2.reshape(count, n, step)
    dw2_ref[:] += mm(act.T, do_ref[:].reshape(count * n, width))


def mlp_a(axa, axb, z0, wvo, mg, ms, w1, b1, w2, b2, d_out):
    half, n, _ = axa.shape
    d = z0.shape[1]
    count = 2
    per = lambda c: lead((count, n, c))
    shifted = lead((count, n, d), lambda i: lax.axis_index('cp') * (half // count) + i)
    return pl.pallas_call(
        mlp_a_kernel,
        grid=(half // count,),
        in_specs=[per(AXW), per(AXW), once((n, d)), once((CPAD, d)), whole((1, d)), whole((1, d)),
                  once((d, d)), whole((1, d)), once((d, d)), whole((1, d)), shifted],
        out_specs=[per(d), per(d), per(d), shifted, once((d, d))],
        out_shape=[
            jax.ShapeDtypeStruct((half, n, d), F32),
            jax.ShapeDtypeStruct((half, n, d), BF16),
            jax.ShapeDtypeStruct((half, n, d), F32),
            jax.ShapeDtypeStruct(d_out.shape, F32),
            jax.ShapeDtypeStruct((d, d), F32),
        ],
        scratch_shapes=[pltpu.VMEM((count * n, d), BF16)],
        compiler_params=params(),
        cost_estimate=cost(2 * half * n * d * (3 * d + 512), half * n * d * 18),
        name="mlp_a",
    )(axa, axb, z0, wvo, mg, ms, w1, b1, w2, b2, d_out)


def mlp_w_kernel(h_ref, slope_ref, do_ref, w2_ref, dpre_ref, dw1_ref, db1_ref):
    @pl.when(pl.program_id(0) == 0)
    def _():
        dw1_ref[:] = jnp.zeros_like(dw1_ref)
        db1_ref[:] = jnp.zeros_like(db1_ref)

    d_act = mm_nt(do_ref[0], w2_ref[:]).astype(BF16).astype(F32)
    d_pre = d_act * slope_ref[0]
    db1_ref[:] += col_sum(d_pre)
    d_pre_low = d_pre.astype(BF16)
    dpre_ref[0] = d_pre_low
    dw1_ref[:] += mm(h_ref[0].T, d_pre_low)


def mlp_w(h, slope, d_out, w2, carries, travel):
    half, n, d = h.shape
    per = lambda c: lead((1, n, c))
    return carrier_call(
        mlp_w_kernel, 5, carries, travel, half,
        [per(d), per(d), lead((1, n, d), lambda i: lax.axis_index('cp') * half + i), whole((d, d))],
        [h, slope, d_out, w2],
        [per(d), whole((d, d)), whole((1, d))],
        [jax.ShapeDtypeStruct((half, n, d), BF16), jax.ShapeDtypeStruct((d, d), F32), jax.ShapeDtypeStruct((1, d), F32)],
        {}, cost(2 * half * n * d * 2 * d, half * n * d * 10))


def mlp_b_kernel(axa_ref, axb_ref, z1_ref, dpre_ref, do_ref, wvo_ref, mg_ref, w1_ref, db1_ref, g_ref, acc_ref):
    ax, top, inv = combine(axa_ref[0], axb_ref[0])
    n, _ = z1_ref.shape[1:]
    z1 = z1_ref[0]
    d_hid = mm_nt(dpre_ref[0], w1_ref[:]).astype(BF16).astype(F32)
    centred = z1 - row_mean(z1)
    rstd = lax.rsqrt(row_mean(centred * centred) + LN_EPS)
    hat = centred * rstd
    d_hat = d_hid * mg_ref[:]
    mean_a = row_mean(d_hat)
    mean_b = row_mean(d_hat * hat)
    d_out = do_ref[0].astype(F32)
    d_mid = d_out + rstd * (d_hat - mean_a - hat * mean_b)
    d_mid_low = d_mid.astype(BF16)

    @pl.when(pl.program_id(0) == 0)
    def _():
        acc_ref[:] = jnp.zeros_like(acc_ref)
        acc_ref[VEC_ROW + 3:VEC_ROW + 4, :] = db1_ref[:]

    p = mm(ax[:, :CPAD].astype(BF16).T, d_mid_low)
    acc_ref[0:n, :] += d_mid
    acc_ref[n:n + CPAD, :] += p
    acc_ref[VEC_ROW:VEC_ROW + 1, :] += col_sum(d_hid * hat)
    acc_ref[VEC_ROW + 1:VEC_ROW + 2, :] += col_sum(d_hid)
    acc_ref[VEC_ROW + 2:VEC_ROW + 3, :] += col_sum(d_out)
    d_ax = jnp.concatenate([mm_nt(d_mid_low, wvo_ref[:]), jnp.zeros((n, AXW - CPAD), F32)], axis=1)
    delta = row_sum(d_ax * ax)
    lane = lax.broadcasted_iota(jnp.int32, d_ax.shape, 1)
    g_ref[0] = jnp.where(lane == SUM_LANE, delta, jnp.where(lane == MAX_LANE, top, jnp.where(lane == INV_LANE, inv, d_ax)))


def mlp_b(axa, axb, z1, dpre, d_out, wvo, mg, w1, db1, carries, travel):
    half, n, _ = axa.shape
    d = z1.shape[2]
    per = lambda c: lead((1, n, c))
    shifted = lead((1, n, d), lambda i: lax.axis_index('cp') * half + i)
    return carrier_call(
        mlp_b_kernel, 1, carries, travel, half,
        [per(AXW), per(AXW), per(d), per(d), shifted, once((CPAD, d)), whole((1, d)), once((d, d)), whole((1, d))],
        [axa, axb, z1, dpre, d_out, wvo, mg, w1, db1],
        [per(AXW), whole((ACC_ROWS, d))],
        [jax.ShapeDtypeStruct((half, n, AXW), F32), jax.ShapeDtypeStruct((ACC_ROWS, d), F32)],
        {}, cost(2 * half * n * d * (d + 800), half * n * d * 10))


def attn_bwd_body(g_ref, ax_ref, e_ref, xn_ref, qpt_ref, t_in_ref, dxn_ref, t_ref):
    g = g_ref[0]
    xn = xn_ref[0]
    e = e_ref[0]
    beta = jnp.exp2(column(ax_ref[0], MAX_LANE) - column(g, MAX_LANE)) * column(g, INV_LANE)
    lane = lax.broadcasted_iota(jnp.int32, g.shape, 1)
    scaled = g * beta
    d_low = jnp.where(lane < CH, scaled, 0.0)[:, :CPAD].astype(BF16)
    d_a = mm(d_low, xn)
    d_s = (e.astype(F32) * (d_a - column(scaled, SUM_LANE))).astype(BF16)

    @pl.when(pl.program_id(0) == 0)
    def _():
        t_ref[:] = jnp.zeros_like(t_ref) if t_in_ref is None else t_in_ref[:]

    t_ref[:] += mm_nt(xn, d_s)
    dxn_ref[0] = (mm(qpt_ref[:], d_s) + mm(d_low.T, e)).astype(BF16)


def attn_bwd(own, g, ax, e, xn, qpt, t_in, dxn_in, ident, carries, travel):
    half, n, m = e.shape
    per = lambda c: lead((1, n, c))

    def at(i):
        core = lax.axis_index('cp')
        return (core if own else 1 - core) * half + i

    shifted = lead((1, CPAD, m), at)
    in_specs = [per(AXW), per(AXW), per(m), shifted, whole((CPAD, n))]
    args = [g, ax, e, xn, qpt]
    aliases = {}
    if not own:
        in_specs += [whole((CPAD, n)), pl.BlockSpec(memory_space=pl.ANY)]
        args += [t_in, dxn_in]
        aliases = {6: 0}

    def body(*refs):
        attn_bwd_body(*refs[:5], None if own else refs[5], *refs[-2:])

    return carrier_call(
        body, ident, carries, travel, half, in_specs, args,
        [shifted, whole((CPAD, n))],
        [jax.ShapeDtypeStruct(xn.shape, BF16), jax.ShapeDtypeStruct((CPAD, n), F32)],
        aliases, cost(8 * half * n * m * 512, half * n * m * 6))


def x_post_kernel(base_ref, gain_ref, x_ref, mean_ref, rstd_ref, dxn_ref, za_ref, zb_ref, wa_ref, wb_ref, full_in_ref, dx_ref, sums_ref, full_ref, w_ref,
                  rows_ref, dg_ref, ds_ref):
    nb, lanes = x_ref.shape[1:]
    pitch = CPAD + ROW_GAP
    late = pl.program_id(0) >= pl.num_programs(0) // 2
    mine = late == (base_ref[0] == 1)

    @pl.when(late)
    def _():
        full_ref[0] = zb_ref[0]

    @pl.when(jnp.logical_not(late))
    def _():
        full_ref[0] = za_ref[0]

    @pl.when(mine)
    def _():
        w_ref[:] = wa_ref[:]

    @pl.when(jnp.logical_not(mine))
    def _():
        w_ref[:] = wb_ref[:]

    for b in range(nb):
        rows_ref[b * pitch:b * pitch + CPAD, :] = dxn_ref[b].astype(F32)
    zero = jnp.zeros((nb, lanes), F32)
    mean = mean_ref[:]
    rstd = rstd_ref[:]

    @pl.when(pl.program_id(0) == 0)
    def _():
        dg_ref[:] = jnp.zeros_like(dg_ref)
        ds_ref[:] = jnp.zeros_like(ds_ref)

    def gather(c, acc):
        da, db = acc
        hat = (x_ref[c].astype(F32) - mean) * rstd
        dxn = rows_ref[pl.ds(c, nb, stride=pitch), :]
        prod = dxn * hat
        dg_ref[c] += prod[:8] + prod[8:]
        ds_ref[c] += dxn[:8] + dxn[8:]
        return da + dxn * gain_ref[c], db + prod * gain_ref[c]

    da, db = lax.fori_loop(0, CH, gather, (zero, zero), unroll=9)
    mean_a = da * (1.0 / CH) * rstd
    mean_b = db * (1.0 / CH) * rstd * rstd

    def put(c, carry):
        centred = x_ref[c].astype(F32) - mean
        dxn = rows_ref[pl.ds(c, nb, stride=pitch), :]
        dx_ref[c] = (dxn * (gain_ref[c] * rstd) - mean_a - centred * mean_b).astype(BF16)
        return carry

    lax.fori_loop(0, CH, put, 0, unroll=9)

    @pl.when(pl.program_id(0) == pl.num_programs(0) - 1)
    def _():
        for k, ref in enumerate((dg_ref, ds_ref)):
            part = jnp.concatenate([jnp.sum(ref[:], axis=1), jnp.zeros((AXW - CH, lanes), F32)], axis=0)
            sums_ref[k:k + 1, :] = jnp.sum(part.T, axis=0, keepdims=True)


def x_post(core, x_gain, x_cm, mean, rstd, dxn, za, zb, full, w_own, w_got):
    _, nb, m = x_cm.shape
    half, n, d = 2 * za.shape[0], *za.shape[1:]
    lanes = m // half
    slab = 2 * w_own.shape[0] // half
    chan = trail((CH, nb, lanes))
    stat = trail((nb, lanes))

    def piece(side):
        last = half // 2 - 1
        return pl.BlockSpec((slab, d), lambda i, core: (
            jnp.clip(i - (core[0] if side else 1 - core[0]) * (half // 2), 0, last), 0))

    return pl.pallas_call(
        x_post_kernel,
        grid_spec=pltpu.PrefetchScalarGridSpec(
            num_scalar_prefetch=1,
            grid=(half,),
            in_specs=[
                pl.BlockSpec(memory_space=pltpu.SMEM),
                chan, stat, stat,
                trail((nb, CPAD, lanes)),
                lead((1, n, d), lambda i: jnp.minimum(i, half // 2 - 1)),
                lead((1, n, d), lambda i: jnp.maximum(i - half // 2, 0)),
                piece(True), piece(False),
                pl.BlockSpec(memory_space=pl.ANY),
            ],
            out_specs=[chan, whole((2, AXW)), pl.BlockSpec((1, n, d), lambda i, core: ((1 - core[0]) * half + i, 0, 0)),
                       lead((slab, d))],
            scratch_shapes=[pltpu.VMEM(((CPAD + ROW_GAP) * nb, lanes), F32),
                            pltpu.VMEM((CH, 8, lanes), F32), pltpu.VMEM((CH, 8, lanes), F32)],
        ),
        out_shape=[
            jax.ShapeDtypeStruct(x_cm.shape, BF16),
            jax.ShapeDtypeStruct((2, AXW), F32),
            jax.ShapeDtypeStruct(full.shape, F32),
            jax.ShapeDtypeStruct((2 * w_own.shape[0], d), F32),
        ],
        input_output_aliases={10: 2},
        compiler_params=params(),
        cost_estimate=cost(6e9, 6 * nb * CH * m + 8 * half * n * d),
        name="x_post",
    )(core, x_gain, x_cm, mean, rstd, dxn, za, zb, w_own, w_got, full)


def finish_kernel(dp, cp, x_ref, t_refs, acc_refs, w_refs, o_ref, outs, got_ref, wholes, send_sem, recv_sem):
    core, x, y, at_core, _, _ = places()
    my_dp = lax.axis_index('dp')
    ids = [(lax.rem(my_dp + i, dp), lax.rem(core + j, cp)) for i in range(dp) for j in range(cp)][1:]
    meet(ids)
    sems = (send_sem, recv_sem)
    copies = [remote(x_ref, got_ref.at[k], sems, k, dev) for k, dev in enumerate(ids)]
    start_all(copies)
    swaps = []
    for k, (buf, parts) in enumerate(zip(wholes, (t_refs, acc_refs, w_refs))):
        half = buf.shape[0] // 2
        if parts is t_refs:
            a, b, c, d = (ref[:] for ref in parts)
            buf[pl.ds(pl.multiple_of(core * half, 8), half), :] = (a + b) + (c + d)
        else:
            eighth = half // 4
            for place, ref in zip((x, 2 + y, 1 - x, 3 - y), parts):
                buf[pl.ds(pl.multiple_of(core * half + place * eighth, 8), eighth), :] = ref[:]
        mine = rows(buf, core * half, half)
        swaps.append(remote(mine, mine, sems, len(ids) + k, at_core))
        swaps[k].start()
    wait_all(copies)
    o_ref[:] = x_ref[:] + jnp.sum(got_ref[:], axis=0)
    for swap, out, buf in zip(swaps, outs, wholes):
        swap.wait()
        out[:] = buf[:]


def finish(mesh, x, t_parts, acc_parts, w_parts):
    count = mesh.size - 1
    shapes = [(k * part[0].shape[0], part[0].shape[1]) for k, part in ((2, t_parts), (8, acc_parts), (8, w_parts))]
    vmem = pl.BlockSpec(memory_space=pltpu.VMEM)

    def kernel(x_ref, *refs):
        finish_kernel(mesh.shape['dp'], mesh.shape['cp'], x_ref, refs[:4], refs[4:8], refs[8:12], refs[12], refs[13:16],
                      refs[16], refs[17:20], *refs[20:])

    return pl.pallas_call(
        kernel,
        in_specs=[vmem] * 13,
        out_specs=[vmem] * 4,
        out_shape=[jax.ShapeDtypeStruct(shape, F32) for shape in (x.shape, *shapes)],
        scratch_shapes=[pltpu.VMEM(shape, F32) for shape in ((count,) + x.shape, *shapes)] + dma_sems(count + 3),
        compiler_params=pltpu.CompilerParams(vmem_limit_bytes=VMEM_LIMIT, collective_id=0, has_side_effects=True),
        name="finish",
    )(x, *t_parts, *acc_parts, *w_parts)


def prologue_kernel(scale, z0_ref, zg_ref, zs_ref, wq_ref, wk_in_ref, wv_in_ref, wo_ref,
                    zn_ref, q_ref, qp_ref, qpt_ref, wvo_ref, wk_ref, wv_ref):
    for src, dst in ((wk_in_ref, wk_ref), (wv_in_ref, wv_ref)):
        dst[256:, :] = jnp.zeros((CPAD - 256, src.shape[1]), BF16)
        dst[:CH, :] = src[:]
    zn = layer_norm(z0_ref[:], zg_ref[:], zs_ref[:]).astype(BF16)
    zn_ref[:] = zn
    q = mm(zn, wq_ref[:]).astype(BF16)
    q_ref[:] = q
    wk = wk_ref[:]
    qp_ref[:] = (mm_nt(q, wk) * (scale * LOG2E)).astype(BF16)
    qpt_ref[:] = (mm_nt(wk, q) * scale).astype(BF16)
    wvo_ref[:] = mm(wv_ref[:], wo_ref[:]).astype(BF16)


def prologue(scale, z0, zg, zs, wq, wk, wv, wo):
    n, d = z0.shape
    vmem = pl.BlockSpec(memory_space=pltpu.VMEM)
    return pl.pallas_call(
        functools.partial(prologue_kernel, scale),
        in_specs=[vmem] * 7,
        out_specs=[vmem] * 7,
        out_shape=[jax.ShapeDtypeStruct(shape, BF16)
                   for shape in ((n, d), (n, d), (n, CPAD), (CPAD, n), (CPAD, d), (CPAD, d), (CPAD, d))],
        compiler_params=pltpu.CompilerParams(vmem_limit_bytes=VMEM_LIMIT),
        cost_estimate=cost(3e9, 12e6),
        name="prologue",
    )(z0, zg, zs, wq, wk, wv, wo)


def final_kernel(scale, t_ref, acc_ref, z0_ref, zg_ref, zn_ref, q_ref, wq_ref, wk_ref, wv_ref, wo_ref,
                 dlat_ref, dzg_ref, dzs_ref, dwq_ref, dwk_ref, dwv_ref, dwo_ref):
    n = z0_ref.shape[0]
    p_low = acc_ref[n:n + CPAD, :].astype(BF16)
    dwo_ref[:] = mm(wv_ref[:].T, p_low)
    dwv_ref[:] = mm_nt(p_low, wo_ref[:])[:CH]
    t_low = (t_ref[:] * scale).astype(BF16)
    dwk_ref[:] = mm(t_low, q_ref[:])[:CH]
    d_q = mm(t_low.T, wk_ref[:]).astype(BF16)
    dwq_ref[:] = mm(zn_ref[:].T, d_q)
    d_zn = mm_nt(d_q, wq_ref[:])
    z0 = z0_ref[:]
    centred = z0 - row_mean(z0)
    rstd = lax.rsqrt(row_mean(centred * centred) + LN_EPS)
    hat = centred * rstd
    dzg_ref[:] = col_sum(d_zn * hat)
    dzs_ref[:] = col_sum(d_zn)
    d_hat = d_zn * zg_ref[:]
    mean_a = row_mean(d_hat)
    mean_b = row_mean(d_hat * hat)
    dlat_ref[:] = acc_ref[:n, :] + rstd * (d_hat - mean_a - hat * mean_b)


def final(scale, t, acc, z0, zg, zn, q, wq, wk, wv, wo):
    n, d = z0.shape
    vmem = pl.BlockSpec(memory_space=pltpu.VMEM)
    shapes = ((n, d), (1, d), (1, d), (d, d), (CH, d), (CH, d), (d, d))
    return pl.pallas_call(
        functools.partial(final_kernel, scale),
        in_specs=[vmem] * 10,
        out_specs=[vmem] * 7,
        out_shape=[jax.ShapeDtypeStruct(shape, F32) for shape in shapes],
        compiler_params=pltpu.CompilerParams(vmem_limit_bytes=VMEM_LIMIT),
        cost_estimate=cost(4e9, 25e6),
        name="final",
    )(t, acc, z0, zg, zn, q, wq, wk, wv, wo)


def solution(mesh):
    x_spec, row_spec = P('dp', 'cp'), P('dp')
    vec_spec = mat_spec = P()
    in_specs = (x_spec, mat_spec, vec_spec, vec_spec, vec_spec, vec_spec, mat_spec, mat_spec, mat_spec, mat_spec,
                vec_spec, vec_spec, mat_spec, vec_spec, mat_spec, vec_spec, row_spec)
    out_specs = (row_spec, x_spec, mat_spec, vec_spec, vec_spec, vec_spec, vec_spec, mat_spec, mat_spec, mat_spec, mat_spec,
                 vec_spec, vec_spec, mat_spec, vec_spec, mat_spec, vec_spec)
    swap = [(0, 1), (1, 0)]

    def step(inputs, latents, x_gain, x_shift, z_gain, z_shift, w_query, w_key, w_value, w_out, m_gain, m_shift, w_up, b_up, w_down, b_down, d_out):
        qk_scale = w_query.shape[1] ** -0.5
        _, d = latents.shape
        half = inputs.shape[0] // 2
        core = lax.axis_index('cp')
        as_ints = lambda *vals: jnp.stack([v.astype(jnp.int32) for v in vals])
        mine = as_ints(core * half, core * (d // 2))
        other = as_ints((1 - core) * half, (1 - core) * (d // 2))
        row = lambda vec: vec.reshape(1, -1)

        x_cm = jnp.transpose(inputs, (2, 0, 1))
        xn, x_mean, x_rstd = x_prep(x_cm, x_gain, x_shift)

        z_norm, queries, qp, qpt, wvo, wk_pad, wv_pad = prologue(
            qk_scale, latents, row(z_gain), row(z_shift), w_query, w_key, w_value, w_out)

        e_other, ax_other = attn_fwd(other, qp, xn, half)
        ax_got = lax.ppermute(ax_other, 'cp', swap)
        e_mine, ax_mine = attn_fwd(mine, qp, xn, half)

        flip = lambda bit: [(k, k ^ bit) for k in range(4)]
        z1, hid, slope, full, dw2 = mlp_a(
            ax_mine, ax_got, latents, wvo, row(m_gain), row(m_shift), w_up, row(b_up), w_down, row(b_down), d_out)
        dpre, dw1, db1, w2_pieces = mlp_w(
            hid, slope, d_out, w_down, [carry(d, d, (0, 1, 2), (0, 2, 6))], [dw2])
        g_mine, acc, w2_half, w1_eighths, za_got = mlp_b(
            ax_mine, ax_got, z1, dpre, d_out, wvo, row(m_gain), w_up, db1,
            [carry(d, d, (3, 4), (0, 2)), carry(d, d, (0, 1), (0, 2)), carry_rows(full.shape, half, 0, half // 2, 2)],
            [w2_pieces, dw1, full])
        g_got = lax.ppermute(g_mine, 'cp', swap)
        dxn, t_part, *w1_eighths, acc_half = attn_bwd(
            True, g_mine, ax_mine, e_mine, xn, qpt, None, None, 3,
            [carry(d, d, (2, 3), (0, 3)), carry(ACC_ROWS, d, (0,), (0,))], [w1_eighths, acc])
        w2_half, dxn = lax.optimization_barrier((w2_half, dxn))
        w2_got = lax.ppermute(w2_half, 'cp', swap)
        dxn, t_part, *acc_eighths, zb_got = attn_bwd(
            False, g_got, ax_other, e_other, xn, qpt, t_part, dxn, 4,
            [carry(ACC_ROWS, d, (1, 2, 3), (0, 5, 7)), carry_rows(full.shape, half, half // 2, half // 2, 0)],
            [acc_half, full])
        w1_eighths, dxn = lax.optimization_barrier((w1_eighths, dxn))

        def halves(own):
            got_x = lax.ppermute(own[0], 'dp', flip(1))
            got_y = lax.ppermute(own[1], 'dp', flip(2))
            return got_x, got_y

        w1_x, w1_y = halves(w1_eighths)
        acc_x, acc_y = halves(acc_eighths)

        t_mine = lax.dynamic_slice_in_dim(t_part, core * (CPAD // 2), CPAD // 2, 0)
        t_send = lax.dynamic_slice_in_dim(t_part, (1 - core) * (CPAD // 2), CPAD // 2, 0)
        t_mine = t_mine + lax.ppermute(t_send, 'cp', swap)
        t_parts = [t_mine]
        for bit in (1, 2, 3):
            t_parts.append(lax.ppermute(t_mine, 'dp', [(k, k ^ bit) for k in range(4)]))
        dx_cm, sums, z_out, d_w_down = x_post(
            core.astype(jnp.int32).reshape(1), x_gain, x_cm, x_mean, x_rstd, dxn, za_got, zb_got, full, w2_half, w2_got)
        sums, t_sum, acc, d_w_up = finish(
            mesh, sums, t_parts, [*acc_eighths, acc_x, acc_y], [*w1_eighths, w1_x, w1_y])
        d_x_gain, d_x_shift = sums[0, :CH], sums[1, :CH]

        d_m_gain, d_m_shift, d_b_down, d_b_up = (acc[VEC_ROW + k] for k in range(4))
        d_lat, d_z_gain, d_z_shift, d_w_query, d_w_key, d_w_value, d_w_out = final(
            qk_scale, t_sum, acc, latents, row(z_gain), z_norm, queries, w_query, wk_pad, wv_pad, w_out)
        return (z_out, jnp.transpose(dx_cm, (1, 2, 0)), d_lat, d_x_gain, d_x_shift, d_z_gain[0], d_z_shift[0],
                d_w_query, d_w_key, d_w_value, d_w_out, d_m_gain, d_m_shift, d_w_up, d_b_up, d_w_down, d_b_down)

    return jax.shard_map(step, mesh=mesh, in_specs=in_specs, out_specs=out_specs, check_vma=False)
```

```python
import functools
import math

import jax
import jax.numpy as jnp
from jax import lax
from jax.experimental import pallas as pl
from jax.experimental.pallas import tpu as pltpu
from jax.sharding import PartitionSpec as P


LN_EPS = 1e-5
F32 = jnp.float32
BF16 = jnp.bfloat16
CH = 261
CPAD = 272
AXW = 384
ROW_GAP = 8
ACC_ROWS = 896
VEC_ROW = 784
SUM_LANE = 261
MAX_LANE = 262
INV_LANE = 263
LOG2E = math.log2(math.e)
GELU_A = math.sqrt(2.0 / math.pi)
GELU_B = 0.044715
VMEM_LIMIT = 63 * 1024 * 1024


def layer_norm(tensor, ln_gain, ln_shift):
    row_mean = jnp.mean(tensor, axis=-1, keepdims=True)
    centred = tensor - row_mean
    variance = jnp.mean(centred * centred, axis=-1, keepdims=True)
    return centred * lax.rsqrt(variance + LN_EPS) * ln_gain + ln_shift


def mm(lhs, rhs):
    return lax.dot_general(lhs, rhs, (((1,), (0,)), ((), ())), preferred_element_type=F32)


def mm_nt(lhs, rhs):
    return lax.dot_general(lhs, rhs, (((1,), (1,)), ((), ())), preferred_element_type=F32)


def params(semantics=1):
    return pltpu.CompilerParams(
        vmem_limit_bytes=VMEM_LIMIT, dimension_semantics=("arbitrary",) * semantics)


def whole(shape, **kw):
    return pl.BlockSpec(shape, lambda *_: (0,) * len(shape), **kw)


def once(shape):
    return whole(shape, pipeline_mode=pl.Buffered(1))


def lead(shape, index=lambda i: i):
    return pl.BlockSpec(shape, lambda i, *_: (index(i),) + (0,) * (len(shape) - 1))


def trail(shape):
    return pl.BlockSpec(shape, lambda i, *_: (0,) * (len(shape) - 1) + (i,))


def row_mean(array):
    return jnp.mean(array, axis=1, keepdims=True)


def row_sum(array):
    return jnp.sum(array, axis=1, keepdims=True)


def col_sum(array):
    return jnp.sum(array, axis=0, keepdims=True)


def column(array, lane):
    return array[:, lane:lane + 1]


def cost(flops, nbytes):
    return pl.CostEstimate(flops=int(flops), bytes_accessed=int(nbytes), transcendentals=0)


def over_channels(term, zero):
    third = CH // 3
    parts = lax.fori_loop(
        0, third, lambda c, acc: tuple(a + term(c + k * third) for k, a in enumerate(acc)), (zero,) * 3, unroll=29)
    return sum(parts[1:], parts[0]) * (1.0 / CH)


def x_prep_kernel(gain_ref, shift_ref, x_ref, xn_ref, mean_ref, rstd_ref, *rows_refs):
    nb, lanes = x_ref.shape[1:]
    pitch = nb + ROW_GAP
    width = lanes // len(rows_refs)
    zero = jnp.zeros((nb, lanes), F32)
    mean = over_channels(lambda c: x_ref[c].astype(F32), zero)

    def square(c):
        d = x_ref[c].astype(F32) - mean
        return d * d

    rstd = lax.rsqrt(over_channels(square, zero) + LN_EPS)
    mean_ref[:] = mean
    rstd_ref[:] = rstd

    def put(c, carry):
        xn = (x_ref[c].astype(F32) - mean) * rstd * gain_ref[c] + shift_ref[c]
        for k, ref in enumerate(rows_refs):
            ref[pl.ds(pl.multiple_of(c * pitch, ROW_GAP), nb), :] = xn[:, k * width:(k + 1) * width]
        return carry

    lax.fori_loop(0, CH, put, 0, unroll=9)
    for k, ref in enumerate(rows_refs):
        ref[CH * pitch:CPAD * pitch, :] = jnp.zeros(((CPAD - CH) * pitch, width), F32)
        for b in range(nb):
            xn_ref[b, :, k * width:(k + 1) * width] = ref[pl.ds(b, CPAD, stride=pitch), :].astype(BF16)


def x_prep(x_cm, x_gain, x_shift):
    _, nb, m = x_cm.shape
    lanes = 256
    return pl.pallas_call(
        x_prep_kernel,
        grid=(m // lanes,),
        in_specs=[
            pl.BlockSpec(memory_space=pltpu.SMEM),
            pl.BlockSpec(memory_space=pltpu.SMEM),
            trail((CH, nb, lanes)),
        ],
        out_specs=[trail((nb, CPAD, lanes)), trail((nb, lanes)), trail((nb, lanes))],
        out_shape=[
            jax.ShapeDtypeStruct((nb, CPAD, m), BF16),
            jax.ShapeDtypeStruct((nb, m), F32),
            jax.ShapeDtypeStruct((nb, m), F32),
        ],
        scratch_shapes=[pltpu.VMEM((CPAD * (nb + ROW_GAP), 128), F32)] * 2,
        compiler_params=params(),
        cost_estimate=cost(3e9, 4 * nb * CH * m),
        name="x_prep",
    )(x_gain, x_shift, x_cm)


def attn_fwd_kernel(base_ref, qp_ref, xn_ref, e_ref, ax_ref):
    xn = xn_ref[0]
    n = qp_ref.shape[0]
    spans = [slice(k * (n // 2), (k + 1) * (n // 2)) for k in range(2)]
    logits = [mm(qp_ref[span, :], xn) for span in spans]
    for span, s in zip(spans, logits):
        top = jnp.max(s, axis=1, keepdims=True)
        e = jnp.exp2(s - top)
        total = row_sum(e)
        e_low = e.astype(BF16)
        e_ref[0, span, :] = e_low
        ax = jnp.concatenate([mm_nt(e_low, xn), jnp.zeros((e.shape[0], AXW - CPAD), F32)], axis=1)
        lane = lax.broadcasted_iota(jnp.int32, ax.shape, 1)
        ax_ref[0, span, :] = jnp.where(lane == SUM_LANE, total, jnp.where(lane == MAX_LANE, top, ax))


def attn_fwd(base, qp, xn, half):
    n = qp.shape[0]
    m = xn.shape[2]
    return pl.pallas_call(
        attn_fwd_kernel,
        grid_spec=pltpu.PrefetchScalarGridSpec(
            num_scalar_prefetch=1,
            grid=(half,),
            in_specs=[
                whole((n, CPAD)),
                pl.BlockSpec((1, CPAD, m), lambda i, base: (base[0] + i, 0, 0)),
            ],
            out_specs=[
                lead((1, n, m)),
                lead((1, n, AXW)),
            ],
        ),
        out_shape=[
            jax.ShapeDtypeStruct((half, n, m), BF16),
            jax.ShapeDtypeStruct((half, n, AXW), F32),
        ],
        compiler_params=params(),
        cost_estimate=cost(4 * half * n * m * 512, half * n * m * 3),
        name="attn_fwd",
    )(base, qp, xn)


def places():
    core, chip = lax.axis_index('cp'), lax.axis_index('dp')
    x, y = lax.rem(chip, 2), chip // 2
    at_x = (y * 2 + (1 - x), core)
    at_y = ((1 - y) * 2 + x, core)
    return core, x, y, (chip, 1 - core), at_x, at_y


def meet(devices):
    barrier = pltpu.get_barrier_semaphore()
    for dev in devices:
        pl.semaphore_signal(barrier, inc=1, device_id=dev, device_id_type=pl.DeviceIdType.MESH)
    pl.semaphore_wait(barrier, len(devices))


def remote(src, dst, sems, k, dev):
    return pltpu.make_async_remote_copy(
        src_ref=src, dst_ref=dst, send_sem=sems[0].at[k], recv_sem=sems[1].at[k],
        device_id=dev, device_id_type=pl.DeviceIdType.MESH)


def rows(ref, start, size):
    return ref.at[pl.ds(pl.multiple_of(start, 8), size)]


def take(ref, start, size):
    return ref[pl.ds(pl.multiple_of(start, 8), size), :]


def at_step(step, when, todo):
    pl.when(step == when)(todo)


def dma_sems(count):
    return [pltpu.SemaphoreType.DMA((count,)), pltpu.SemaphoreType.DMA((count,))]


class Carry:
    def __init__(self, in_shape, in_hbm, out_shapes, scratch, head, tail, out_hbm=False):
        self.in_shape, self.in_hbm, self.out_shapes, self.scratch = in_shape, in_hbm, out_shapes, scratch
        self.out_hbm = out_hbm
        self.head, self.tail = head, tail


def start_all(copies):
    for copy in copies:
        copy.start()


def wait_all(copies):
    for copy in copies:
        copy.wait()


class Plan:
    def __init__(self, total):
        self.half, self.quarter, self.eighth, self.part = (total // k for k in (2, 4, 8, 16))
        self.core, self.x, self.y, self.at_core, self.at_x, self.at_y = places()
        self.spot = (self.x * self.eighth, self.quarter + self.y * self.eighth)
        self.away = ((1 - self.x) * self.eighth, self.quarter + (1 - self.y) * self.eighth)
        self.fine = (self.y * self.part, self.x * self.part)
        self.fine_away = ((1 - self.y) * self.part, (1 - self.x) * self.part)
        self.first, self.second = (self.at_x, self.at_y), (self.at_y, self.at_x)


def carry(total, width, stages, at):
    half, _, eighth, part = (total // k for k in (2, 4, 8, 16))
    lo, hi = stages[0], stages[-1]
    in_shape = {0: (total, width), 1: (half, width), 2: (2, eighth, width), 3: (2, part, width)}[lo]
    out_shape = {0: (half, width), 1: (2, eighth, width), 2: (2, part, width), 3: (eighth, width), 4: (half, width)}[hi]
    shapes = {}
    if 0 in stages:
        shapes.update(half=(half, width), rx0=(half, width))
    if 1 in stages:
        shapes.update(rx1=(2, eighth, width))
    if 2 in stages:
        shapes.update(rx2=(2, part, width))
    if 1 in stages and 2 in stages:
        shapes.update(mid=(2, eighth, width))
    if 2 in stages and 3 in stages:
        shapes.update(fin=(2, part, width))
    if 3 in stages:
        shapes.update(buf=(2, eighth, width))
    if 4 in stages:
        shapes.update(full=(half, width))
    names = list(shapes)
    count = 2 * len(stages)
    scratch = [pltpu.VMEM(shape, F32) for shape in shapes.values()] + [pltpu.SemaphoreType.DMA((1,))] + dma_sems(count)

    def build(src, refs):
        r = dict(zip(names, refs))
        local, sems = refs[-3], (refs[-2], refs[-1])
        p = Plan(total)
        slot = lambda stage, k: 2 * (stage - lo) + k
        two = (0, 1)
        moves = {}
        if 0 in stages:
            moves[0] = lambda: [pltpu.make_async_copy(rows(src, p.core * half, half), r['half'], local.at[0]),
                                remote(rows(src, (1 - p.core) * half, half), r['rx0'], sems, slot(0, 0), p.at_core)]
        if 1 in stages:
            pair = r.get('half', src)
            moves[1] = lambda: [remote(rows(pair, p.away[k], eighth), r['rx1'].at[k], sems, slot(1, k), p.first[k])
                                for k in two]
        if 2 in stages:
            mid = r.get('mid', src)
            moves[2] = lambda: [remote(rows(mid.at[k], p.fine_away[k], part), r['rx2'].at[k], sems, slot(2, k), p.second[k])
                                for k in two]
        if 3 in stages:
            fin = r.get('fin', src)
            moves[3] = lambda: [remote(fin.at[k], rows(r['buf'].at[k], p.fine[k], part), sems, slot(3, k), p.second[k])
                                for k in two]
        if 4 in stages:
            moves[4] = lambda: [remote(r['buf'].at[k], rows(r['full'], p.spot[k], eighth), sems, slot(4, k), p.first[k])
                                for k in two]

        def before(stage):
            if stage == 3:
                for k in two:
                    r['buf'][k, pl.ds(pl.multiple_of(p.fine[k], 8), part), :] = fin[k]

        def after(stage, out):
            wait_all(moves[stage]())
            if stage == 0:
                r['half'][:] += r['rx0'][:]
                if hi == 0:
                    out[:] = r['half'][:]
            elif stage == 1:
                dst = out if hi == 1 else r['mid']
                for k in two:
                    dst[k] = take(pair, p.spot[k], eighth) + r['rx1'][k]
            elif stage == 2:
                dst = out if hi == 2 else r['fin']
                for k in two:
                    dst[k] = take(mid.at[k], p.fine[k], part) + r['rx2'][k]
            elif stage == 3 and hi == 3:
                for k in two:
                    out[k][:] = r['buf'][k]
            elif stage == 4:
                for k in two:
                    r['full'][pl.ds(pl.multiple_of(p.spot[k], 8), eighth), :] = r['buf'][k]
                out[:] = r['full'][:]

        return moves, before, after

    def head(step, src, outs, refs):
        out = outs if hi == 3 else outs[0]
        for stage, when in zip(stages, at):
            def go(stage=stage):
                moves, before, after = build(src, refs)
                if stage > lo:
                    after(stage - 1, out)
                before(stage)
                start_all(moves[stage]())

            at_step(step, when, go)

    def tail(src, outs, refs):
        build(src, refs)[2](hi, outs if hi == 3 else outs[0])

    return Carry(in_shape, lo == 0, [out_shape] * (2 if hi == 3 else 1), scratch, head, tail)


def carry_rows(shape, half, start, count, when):
    def move(src, outs, refs):
        core, _, _, at_core, _, _ = places()
        return remote(src.at[pl.ds(core * half + start, count)], outs[0], refs, 0, at_core)

    def head(step, src, outs, refs):
        at_step(step, when, lambda: move(src, outs, refs).start())

    def tail(src, outs, refs):
        move(src, outs, refs).wait()

    return Carry(shape, True, [(count,) + shape[1:]], dma_sems(1), head, tail, True)


def carrier_call(body, ident, carries, travel, grid, in_specs, args, out_specs, out_shape, aliases, cost_estimate):
    n_in, n_out, n_c = len(in_specs), len(out_specs), len(carries)
    c_in = [pl.BlockSpec(memory_space=pl.ANY) if c.in_hbm else whole(c.in_shape) for c in carries]

    def kernel(*refs):
        ins, c_ins = refs[:n_in], refs[n_in:n_in + n_c]
        rest = refs[n_in + n_c:]
        outs, scratch = rest[:n_out], rest[n_out + sum(len(c.out_shapes) for c in carries):]
        rest = rest[n_out:]
        c_outs, parts = [], []
        for c in carries:
            c_outs.append(rest[:len(c.out_shapes)])
            rest = rest[len(c.out_shapes):]
            parts.append(scratch[:len(c.scratch)])
            scratch = scratch[len(c.scratch):]
        step = pl.program_id(0)

        @pl.when(step == 0)
        def _():
            _, _, _, at_core, at_x, at_y = places()
            meet((at_core, at_x, at_y))

        for c, src, out, refs_c in zip(carries, c_ins, c_outs, parts):
            c.head(step, src, out, refs_c)
        body(*ins, *outs)

        @pl.when(step == grid - 1)
        def _():
            for c, src, out, refs_c in zip(carries, c_ins, c_outs, parts):
                c.tail(src, out, refs_c)

    return pl.pallas_call(
        kernel,
        grid=(grid,),
        in_specs=in_specs + c_in,
        out_specs=out_specs + [pl.BlockSpec(memory_space=pl.ANY) if c.out_hbm else whole(shape)
                               for c in carries for shape in c.out_shapes],
        out_shape=out_shape + [jax.ShapeDtypeStruct(shape, F32) for c in carries for shape in c.out_shapes],
        scratch_shapes=[shape for c in carries for shape in c.scratch],
        input_output_aliases=aliases,
        compiler_params=pltpu.CompilerParams(
            vmem_limit_bytes=VMEM_LIMIT, dimension_semantics=("arbitrary",), collective_id=ident,
            has_side_effects=True),
        cost_estimate=cost_estimate,
    )(*args, *travel)


def combine(mine, other):
    top_a, top_b = column(mine, MAX_LANE), column(other, MAX_LANE)
    top = jnp.maximum(top_a, top_b)
    fa, fb = jnp.exp2(top_a - top), jnp.exp2(top_b - top)
    inv = 1.0 / (column(mine, SUM_LANE) * fa + column(other, SUM_LANE) * fb)
    ax = mine * (fa * inv) + other * (fb * inv)
    lane = lax.broadcasted_iota(jnp.int32, ax.shape, 1)
    return jnp.where(lane < CH, ax, 0.0), top, inv


def mlp_a_kernel(axa_ref, axb_ref, z0_ref, wvo_ref, mg_ref, ms_ref, w1_ref, b1_ref, w2_ref, b2_ref, do_ref,
                 z1_ref, h_ref, slope_ref, full_ref, dw2_ref, act_ref):
    count, n, width = z1_ref.shape
    step = 512
    flat = lambda ref, cols: ref[:, :, cols].reshape(count * n, step)

    @pl.when(pl.program_id(0) == 0)
    def _():
        dw2_ref[:] = jnp.zeros_like(dw2_ref)

    for b in range(count):
        ax, _, _ = combine(axa_ref[b], axb_ref[b])
        z1 = z0_ref[:] + mm(ax[:, :CPAD].astype(BF16), wvo_ref[:])
        z1_ref[b] = z1
        h_ref[b] = layer_norm(z1, mg_ref[:], ms_ref[:]).astype(BF16)
    h = h_ref[:].reshape(count * n, width)
    spans = [slice(lo, lo + step) for lo in range(0, width, step)]
    for cols in spans:
        pre = mm(h, w1_ref[:, cols]) + b1_ref[:, cols]
        sq = pre * pre
        t = jnp.tanh(pre * (GELU_A + (GELU_A * GELU_B) * sq))
        half_t = 0.5 + 0.5 * t
        act_ref[:, cols] = (pre * half_t).astype(BF16)
        slope = half_t + (0.5 * pre) * (1.0 - t * t) * (GELU_A + (3.0 * GELU_A * GELU_B) * sq)
        slope_ref[:, :, cols] = slope.reshape(count, n, step)
    act = act_ref[:]
    for cols in spans:
        z2 = flat(z1_ref, cols) + mm(act, w2_ref[:, cols]) + b2_ref[:, cols]
        full_ref[:, :, cols] = z2.reshape(count, n, step)
    dw2_ref[:] += mm(act.T, do_ref[:].reshape(count * n, width))


def mlp_a(axa, axb, z0, wvo, mg, ms, w1, b1, w2, b2, d_out):
    half, n, _ = axa.shape
    d = z0.shape[1]
    count = 2
    per = lambda c: lead((count, n, c))
    shifted = lead((count, n, d), lambda i: lax.axis_index('cp') * (half // count) + i)
    return pl.pallas_call(
        mlp_a_kernel,
        grid=(half // count,),
        in_specs=[per(AXW), per(AXW), once((n, d)), once((CPAD, d)), whole((1, d)), whole((1, d)),
                  once((d, d)), whole((1, d)), once((d, d)), whole((1, d)), shifted],
        out_specs=[per(d), per(d), per(d), shifted, once((d, d))],
        out_shape=[
            jax.ShapeDtypeStruct((half, n, d), F32),
            jax.ShapeDtypeStruct((half, n, d), BF16),
            jax.ShapeDtypeStruct((half, n, d), F32),
            jax.ShapeDtypeStruct(d_out.shape, F32),
            jax.ShapeDtypeStruct((d, d), F32),
        ],
        scratch_shapes=[pltpu.VMEM((count * n, d), BF16)],
        compiler_params=params(),
        cost_estimate=cost(2 * half * n * d * (3 * d + 512), half * n * d * 18),
        name="mlp_a",
    )(axa, axb, z0, wvo, mg, ms, w1, b1, w2, b2, d_out)


def mlp_w_kernel(h_ref, slope_ref, do_ref, w2_ref, dpre_ref, dw1_ref, db1_ref):
    @pl.when(pl.program_id(0) == 0)
    def _():
        dw1_ref[:] = jnp.zeros_like(dw1_ref)
        db1_ref[:] = jnp.zeros_like(db1_ref)

    d_act = mm_nt(do_ref[0], w2_ref[:]).astype(BF16).astype(F32)
    d_pre = d_act * slope_ref[0]
    db1_ref[:] += col_sum(d_pre)
    d_pre_low = d_pre.astype(BF16)
    dpre_ref[0] = d_pre_low
    dw1_ref[:] += mm(h_ref[0].T, d_pre_low)


def mlp_w(h, slope, d_out, w2, carries, travel):
    half, n, d = h.shape
    per = lambda c: lead((1, n, c))
    return carrier_call(
        mlp_w_kernel, 5, carries, travel, half,
        [per(d), per(d), lead((1, n, d), lambda i: lax.axis_index('cp') * half + i), whole((d, d))],
        [h, slope, d_out, w2],
        [per(d), whole((d, d)), whole((1, d))],
        [jax.ShapeDtypeStruct((half, n, d), BF16), jax.ShapeDtypeStruct((d, d), F32), jax.ShapeDtypeStruct((1, d), F32)],
        {}, cost(2 * half * n * d * 2 * d, half * n * d * 10))


def mlp_b_kernel(axa_ref, axb_ref, z1_ref, dpre_ref, do_ref, wvo_ref, mg_ref, w1_ref, db1_ref, g_ref, acc_ref):
    ax, top, inv = combine(axa_ref[0], axb_ref[0])
    n, _ = z1_ref.shape[1:]
    z1 = z1_ref[0]
    d_hid = mm_nt(dpre_ref[0], w1_ref[:]).astype(BF16).astype(F32)
    centred = z1 - row_mean(z1)
    rstd = lax.rsqrt(row_mean(centred * centred) + LN_EPS)
    hat = centred * rstd
    d_hat = d_hid * mg_ref[:]
    mean_a = row_mean(d_hat)
    mean_b = row_mean(d_hat * hat)
    d_out = do_ref[0].astype(F32)
    d_mid = d_out + rstd * (d_hat - mean_a - hat * mean_b)
    d_mid_low = d_mid.astype(BF16)

    @pl.when(pl.program_id(0) == 0)
    def _():
        acc_ref[:] = jnp.zeros_like(acc_ref)
        acc_ref[VEC_ROW + 3:VEC_ROW + 4, :] = db1_ref[:]

    p = mm(ax[:, :CPAD].astype(BF16).T, d_mid_low)
    acc_ref[0:n, :] += d_mid
    acc_ref[n:n + CPAD, :] += p
    acc_ref[VEC_ROW:VEC_ROW + 1, :] += col_sum(d_hid * hat)
    acc_ref[VEC_ROW + 1:VEC_ROW + 2, :] += col_sum(d_hid)
    acc_ref[VEC_ROW + 2:VEC_ROW + 3, :] += col_sum(d_out)
    d_ax = jnp.concatenate([mm_nt(d_mid_low, wvo_ref[:]), jnp.zeros((n, AXW - CPAD), F32)], axis=1)
    delta = row_sum(d_ax * ax)
    lane = lax.broadcasted_iota(jnp.int32, d_ax.shape, 1)
    g_ref[0] = jnp.where(lane == SUM_LANE, delta, jnp.where(lane == MAX_LANE, top, jnp.where(lane == INV_LANE, inv, d_ax)))


def mlp_b(axa, axb, z1, dpre, d_out, wvo, mg, w1, db1, carries, travel):
    half, n, _ = axa.shape
    d = z1.shape[2]
    per = lambda c: lead((1, n, c))
    shifted = lead((1, n, d), lambda i: lax.axis_index('cp') * half + i)
    return carrier_call(
        mlp_b_kernel, 1, carries, travel, half,
        [per(AXW), per(AXW), per(d), per(d), shifted, once((CPAD, d)), whole((1, d)), once((d, d)), whole((1, d))],
        [axa, axb, z1, dpre, d_out, wvo, mg, w1, db1],
        [per(AXW), whole((ACC_ROWS, d))],
        [jax.ShapeDtypeStruct((half, n, AXW), F32), jax.ShapeDtypeStruct((ACC_ROWS, d), F32)],
        {}, cost(2 * half * n * d * (d + 800), half * n * d * 10))


def attn_bwd_body(g_ref, ax_ref, e_ref, xn_ref, qpt_ref, t_in_ref, dxn_ref, t_ref):
    g = g_ref[0]
    xn = xn_ref[0]
    e = e_ref[0]
    beta = jnp.exp2(column(ax_ref[0], MAX_LANE) - column(g, MAX_LANE)) * column(g, INV_LANE)
    lane = lax.broadcasted_iota(jnp.int32, g.shape, 1)
    scaled = g * beta
    d_low = jnp.where(lane < CH, scaled, 0.0)[:, :CPAD].astype(BF16)
    d_a = mm(d_low, xn)
    d_s = (e.astype(F32) * (d_a - column(scaled, SUM_LANE))).astype(BF16)

    @pl.when(pl.program_id(0) == 0)
    def _():
        t_ref[:] = jnp.zeros_like(t_ref) if t_in_ref is None else t_in_ref[:]

    t_ref[:] += mm_nt(xn, d_s)
    dxn_ref[0] = (mm(qpt_ref[:], d_s) + mm(d_low.T, e)).astype(BF16)


def attn_bwd(own, g, ax, e, xn, qpt, t_in, dxn_in, ident, carries, travel):
    half, n, m = e.shape
    per = lambda c: lead((1, n, c))

    def at(i):
        core = lax.axis_index('cp')
        return (core if own else 1 - core) * half + i

    shifted = lead((1, CPAD, m), at)
    in_specs = [per(AXW), per(AXW), per(m), shifted, whole((CPAD, n))]
    args = [g, ax, e, xn, qpt]
    aliases = {}
    if not own:
        in_specs += [whole((CPAD, n)), pl.BlockSpec(memory_space=pl.ANY)]
        args += [t_in, dxn_in]
        aliases = {6: 0}

    def body(*refs):
        attn_bwd_body(*refs[:5], None if own else refs[5], *refs[-2:])

    return carrier_call(
        body, ident, carries, travel, half, in_specs, args,
        [shifted, whole((CPAD, n))],
        [jax.ShapeDtypeStruct(xn.shape, BF16), jax.ShapeDtypeStruct((CPAD, n), F32)],
        aliases, cost(8 * half * n * m * 512, half * n * m * 6))


def x_post_kernel(base_ref, gain_ref, x_ref, mean_ref, rstd_ref, dxn_ref, za_ref, zb_ref, wa_ref, wb_ref, full_in_ref, dx_ref, sums_ref, full_ref, w_ref,
                  rows_ref, dg_ref, ds_ref):
    nb, lanes = x_ref.shape[1:]
    pitch = CPAD + ROW_GAP
    late = pl.program_id(0) >= pl.num_programs(0) // 2
    mine = late == (base_ref[0] == 1)

    @pl.when(late)
    def _():
        full_ref[0] = zb_ref[0]

    @pl.when(jnp.logical_not(late))
    def _():
        full_ref[0] = za_ref[0]

    @pl.when(mine)
    def _():
        w_ref[:] = wa_ref[:]

    @pl.when(jnp.logical_not(mine))
    def _():
        w_ref[:] = wb_ref[:]

    for b in range(nb):
        rows_ref[b * pitch:b * pitch + CPAD, :] = dxn_ref[b].astype(F32)
    zero = jnp.zeros((nb, lanes), F32)
    mean = mean_ref[:]
    rstd = rstd_ref[:]

    @pl.when(pl.program_id(0) == 0)
    def _():
        dg_ref[:] = jnp.zeros_like(dg_ref)
        ds_ref[:] = jnp.zeros_like(ds_ref)

    def gather(c, acc):
        da, db = acc
        hat = (x_ref[c].astype(F32) - mean) * rstd
        dxn = rows_ref[pl.ds(c, nb, stride=pitch), :]
        prod = dxn * hat
        dg_ref[c] += prod[:8] + prod[8:]
        ds_ref[c] += dxn[:8] + dxn[8:]
        return da + dxn * gain_ref[c], db + prod * gain_ref[c]

    da, db = lax.fori_loop(0, CH, gather, (zero, zero), unroll=29)
    mean_a = da * (1.0 / CH) * rstd
    mean_b = db * (1.0 / CH) * rstd * rstd

    def put(c, carry):
        centred = x_ref[c].astype(F32) - mean
        dxn = rows_ref[pl.ds(c, nb, stride=pitch), :]
        dx_ref[c] = (dxn * (gain_ref[c] * rstd) - mean_a - centred * mean_b).astype(BF16)
        return carry

    lax.fori_loop(0, CH, put, 0, unroll=29)

    @pl.when(pl.program_id(0) == pl.num_programs(0) - 1)
    def _():
        for k, ref in enumerate((dg_ref, ds_ref)):
            part = jnp.concatenate([jnp.sum(ref[:], axis=1), jnp.zeros((AXW - CH, lanes), F32)], axis=0)
            sums_ref[k:k + 1, :] = jnp.sum(part.T, axis=0, keepdims=True)


def x_post(core, x_gain, x_cm, mean, rstd, dxn, za, zb, full, w_own, w_got):
    _, nb, m = x_cm.shape
    half, n, d = 2 * za.shape[0], *za.shape[1:]
    lanes = m // half
    slab = 2 * w_own.shape[0] // half
    chan = trail((CH, nb, lanes))
    stat = trail((nb, lanes))

    def piece(side):
        last = half // 2 - 1
        return pl.BlockSpec((slab, d), lambda i, core: (
            jnp.clip(i - (core[0] if side else 1 - core[0]) * (half // 2), 0, last), 0))

    return pl.pallas_call(
        x_post_kernel,
        grid_spec=pltpu.PrefetchScalarGridSpec(
            num_scalar_prefetch=1,
            grid=(half,),
            in_specs=[
                pl.BlockSpec(memory_space=pltpu.SMEM),
                chan, stat, stat,
                trail((nb, CPAD, lanes)),
                lead((1, n, d), lambda i: jnp.minimum(i, half // 2 - 1)),
                lead((1, n, d), lambda i: jnp.maximum(i - half // 2, 0)),
                piece(True), piece(False),
                pl.BlockSpec(memory_space=pl.ANY),
            ],
            out_specs=[chan, whole((2, AXW)), pl.BlockSpec((1, n, d), lambda i, core: ((1 - core[0]) * half + i, 0, 0)),
                       lead((slab, d))],
            scratch_shapes=[pltpu.VMEM(((CPAD + ROW_GAP) * nb, lanes), F32),
                            pltpu.VMEM((CH, 8, lanes), F32), pltpu.VMEM((CH, 8, lanes), F32)],
        ),
        out_shape=[
            jax.ShapeDtypeStruct(x_cm.shape, BF16),
            jax.ShapeDtypeStruct((2, AXW), F32),
            jax.ShapeDtypeStruct(full.shape, F32),
            jax.ShapeDtypeStruct((2 * w_own.shape[0], d), F32),
        ],
        input_output_aliases={10: 2},
        compiler_params=params(),
        cost_estimate=cost(6e9, 6 * nb * CH * m + 8 * half * n * d),
        name="x_post",
    )(core, x_gain, x_cm, mean, rstd, dxn, za, zb, w_own, w_got, full)


def finish_kernel(dp, cp, x_ref, t_refs, acc_refs, w_refs, o_ref, outs, got_ref, wholes, send_sem, recv_sem):
    core, x, y, at_core, _, _ = places()
    my_dp = lax.axis_index('dp')
    ids = [(lax.rem(my_dp + i, dp), lax.rem(core + j, cp)) for i in range(dp) for j in range(cp)][1:]
    meet(ids)
    sems = (send_sem, recv_sem)
    copies = [remote(x_ref, got_ref.at[k], sems, k, dev) for k, dev in enumerate(ids)]
    start_all(copies)
    swaps = []
    for k, (buf, parts) in enumerate(zip(wholes, (t_refs, acc_refs, w_refs))):
        half = buf.shape[0] // 2
        if parts is t_refs:
            a, b, c, d = (ref[:] for ref in parts)
            buf[pl.ds(pl.multiple_of(core * half, 8), half), :] = (a + b) + (c + d)
        else:
            eighth = half // 4
            for place, ref in zip((x, 2 + y, 1 - x, 3 - y), parts):
                buf[pl.ds(pl.multiple_of(core * half + place * eighth, 8), eighth), :] = ref[:]
        mine = rows(buf, core * half, half)
        swaps.append(remote(mine, mine, sems, len(ids) + k, at_core))
        swaps[k].start()
    wait_all(copies)
    o_ref[:] = x_ref[:] + jnp.sum(got_ref[:], axis=0)
    for swap, out, buf in zip(swaps, outs, wholes):
        swap.wait()
        out[:] = buf[:]


def finish(mesh, x, t_parts, acc_parts, w_parts):
    count = mesh.size - 1
    shapes = [(k * part[0].shape[0], part[0].shape[1]) for k, part in ((2, t_parts), (8, acc_parts), (8, w_parts))]
    vmem = pl.BlockSpec(memory_space=pltpu.VMEM)

    def kernel(x_ref, *refs):
        finish_kernel(mesh.shape['dp'], mesh.shape['cp'], x_ref, refs[:4], refs[4:8], refs[8:12], refs[12], refs[13:16],
                      refs[16], refs[17:20], *refs[20:])

    return pl.pallas_call(
        kernel,
        in_specs=[vmem] * 13,
        out_specs=[vmem] * 4,
        out_shape=[jax.ShapeDtypeStruct(shape, F32) for shape in (x.shape, *shapes)],
        scratch_shapes=[pltpu.VMEM(shape, F32) for shape in ((count,) + x.shape, *shapes)] + dma_sems(count + 3),
        compiler_params=pltpu.CompilerParams(vmem_limit_bytes=VMEM_LIMIT, collective_id=0, has_side_effects=True),
        name="finish",
    )(x, *t_parts, *acc_parts, *w_parts)


def prologue_kernel(scale, z0_ref, zg_ref, zs_ref, wq_ref, wk_in_ref, wv_in_ref, wo_ref,
                    zn_ref, q_ref, qp_ref, qpt_ref, wvo_ref, wk_ref, wv_ref):
    for src, dst in ((wk_in_ref, wk_ref), (wv_in_ref, wv_ref)):
        dst[256:, :] = jnp.zeros((CPAD - 256, src.shape[1]), BF16)
        dst[:CH, :] = src[:]
    zn = layer_norm(z0_ref[:], zg_ref[:], zs_ref[:]).astype(BF16)
    zn_ref[:] = zn
    q = mm(zn, wq_ref[:]).astype(BF16)
    q_ref[:] = q
    wk = wk_ref[:]
    qp_ref[:] = (mm_nt(q, wk) * (scale * LOG2E)).astype(BF16)
    qpt_ref[:] = (mm_nt(wk, q) * scale).astype(BF16)
    wvo_ref[:] = mm(wv_ref[:], wo_ref[:]).astype(BF16)


def prologue(scale, z0, zg, zs, wq, wk, wv, wo):
    n, d = z0.shape
    vmem = pl.BlockSpec(memory_space=pltpu.VMEM)
    return pl.pallas_call(
        functools.partial(prologue_kernel, scale),
        in_specs=[vmem] * 7,
        out_specs=[vmem] * 7,
        out_shape=[jax.ShapeDtypeStruct(shape, BF16)
                   for shape in ((n, d), (n, d), (n, CPAD), (CPAD, n), (CPAD, d), (CPAD, d), (CPAD, d))],
        compiler_params=pltpu.CompilerParams(vmem_limit_bytes=VMEM_LIMIT),
        cost_estimate=cost(3e9, 12e6),
        name="prologue",
    )(z0, zg, zs, wq, wk, wv, wo)


def final_kernel(scale, t_ref, acc_ref, z0_ref, zg_ref, zn_ref, q_ref, wq_ref, wk_ref, wv_ref, wo_ref, dw1_ref,
                 dlat_ref, dzg_ref, dzs_ref, dwq_ref, dwk_ref, dwv_ref, dwo_ref, dw_up_ref):
    n = z0_ref.shape[0]
    dw_up_ref[:] = dw1_ref[:]
    p_low = acc_ref[n:n + CPAD, :].astype(BF16)
    dwo_ref[:] = mm(wv_ref[:].T, p_low)
    dwv_ref[:] = mm_nt(p_low, wo_ref[:])[:CH]
    t_low = (t_ref[:] * scale).astype(BF16)
    dwk_ref[:] = mm(t_low, q_ref[:])[:CH]
    d_q = mm(t_low.T, wk_ref[:]).astype(BF16)
    dwq_ref[:] = mm(zn_ref[:].T, d_q)
    d_zn = mm_nt(d_q, wq_ref[:])
    z0 = z0_ref[:]
    centred = z0 - row_mean(z0)
    rstd = lax.rsqrt(row_mean(centred * centred) + LN_EPS)
    hat = centred * rstd
    dzg_ref[:] = col_sum(d_zn * hat)
    dzs_ref[:] = col_sum(d_zn)
    d_hat = d_zn * zg_ref[:]
    mean_a = row_mean(d_hat)
    mean_b = row_mean(d_hat * hat)
    dlat_ref[:] = acc_ref[:n, :] + rstd * (d_hat - mean_a - hat * mean_b)


def final(scale, t, acc, z0, zg, zn, q, wq, wk, wv, wo, dw1):
    n, d = z0.shape
    vmem = pl.BlockSpec(memory_space=pltpu.VMEM)
    shapes = ((n, d), (1, d), (1, d), (d, d), (CH, d), (CH, d), (d, d), (d, d))
    return pl.pallas_call(
        functools.partial(final_kernel, scale),
        in_specs=[vmem] * 11,
        out_specs=[vmem] * 8,
        out_shape=[jax.ShapeDtypeStruct(shape, F32) for shape in shapes],
        compiler_params=pltpu.CompilerParams(vmem_limit_bytes=VMEM_LIMIT),
        cost_estimate=cost(4e9, 25e6),
        name="final",
    )(t, acc, z0, zg, zn, q, wq, wk, wv, wo, dw1)


def solution(mesh):
    x_spec, row_spec = P('dp', 'cp'), P('dp')
    vec_spec = mat_spec = P()
    in_specs = (x_spec, mat_spec, vec_spec, vec_spec, vec_spec, vec_spec, mat_spec, mat_spec, mat_spec, mat_spec,
                vec_spec, vec_spec, mat_spec, vec_spec, mat_spec, vec_spec, row_spec)
    out_specs = (row_spec, x_spec, mat_spec, vec_spec, vec_spec, vec_spec, vec_spec, mat_spec, mat_spec, mat_spec, mat_spec,
                 vec_spec, vec_spec, mat_spec, vec_spec, mat_spec, vec_spec)
    swap = [(0, 1), (1, 0)]

    def step(inputs, latents, x_gain, x_shift, z_gain, z_shift, w_query, w_key, w_value, w_out, m_gain, m_shift, w_up, b_up, w_down, b_down, d_out):
        qk_scale = w_query.shape[1] ** -0.5
        _, d = latents.shape
        half = inputs.shape[0] // 2
        core = lax.axis_index('cp')
        as_ints = lambda *vals: jnp.stack([v.astype(jnp.int32) for v in vals])
        mine = as_ints(core * half, core * (d // 2))
        other = as_ints((1 - core) * half, (1 - core) * (d // 2))
        row = lambda vec: vec.reshape(1, -1)

        x_cm = jnp.transpose(inputs, (2, 0, 1))
        xn, x_mean, x_rstd = x_prep(x_cm, x_gain, x_shift)

        z_norm, queries, qp, qpt, wvo, wk_pad, wv_pad = prologue(
            qk_scale, latents, row(z_gain), row(z_shift), w_query, w_key, w_value, w_out)

        e_other, ax_other = attn_fwd(other, qp, xn, half)
        ax_got = lax.ppermute(ax_other, 'cp', swap)
        e_mine, ax_mine = attn_fwd(mine, qp, xn, half)

        flip = lambda bit: [(k, k ^ bit) for k in range(4)]
        z1, hid, slope, full, dw2 = mlp_a(
            ax_mine, ax_got, latents, wvo, row(m_gain), row(m_shift), w_up, row(b_up), w_down, row(b_down), d_out)
        dpre, dw1, db1, w2_pieces = mlp_w(
            hid, slope, d_out, w_down, [carry(d, d, (0, 1, 2), (0, 2, 6))], [dw2])
        g_mine, acc, w2_half, w1_eighths, za_got = mlp_b(
            ax_mine, ax_got, z1, dpre, d_out, wvo, row(m_gain), w_up, db1,
            [carry(d, d, (3, 4), (0, 2)), carry(d, d, (0, 1), (0, 2)), carry_rows(full.shape, half, 0, half // 2, 2)],
            [w2_pieces, dw1, full])
        g_got = lax.ppermute(g_mine, 'cp', swap)
        dxn, t_part, *w1_eighths, acc_half = attn_bwd(
            True, g_mine, ax_mine, e_mine, xn, qpt, None, None, 3,
            [carry(d, d, (2, 3), (0, 3)), carry(ACC_ROWS, d, (0,), (0,))], [w1_eighths, acc])
        w2_half, dxn = lax.optimization_barrier((w2_half, dxn))
        w2_got = lax.ppermute(w2_half, 'cp', swap)
        dxn, t_part, *acc_eighths, zb_got = attn_bwd(
            False, g_got, ax_other, e_other, xn, qpt, t_part, dxn, 4,
            [carry(ACC_ROWS, d, (1, 2, 3), (0, 5, 7)), carry_rows(full.shape, half, half // 2, half // 2, 0)],
            [acc_half, full])
        w1_eighths, dxn = lax.optimization_barrier((w1_eighths, dxn))

        def halves(own):
            got_x = lax.ppermute(own[0], 'dp', flip(1))
            got_y = lax.ppermute(own[1], 'dp', flip(2))
            return got_x, got_y

        w1_x, w1_y = halves(w1_eighths)
        acc_x, acc_y = halves(acc_eighths)

        t_mine = lax.dynamic_slice_in_dim(t_part, core * (CPAD // 2), CPAD // 2, 0)
        t_send = lax.dynamic_slice_in_dim(t_part, (1 - core) * (CPAD // 2), CPAD // 2, 0)
        t_mine = t_mine + lax.ppermute(t_send, 'cp', swap)
        t_parts = [t_mine]
        for bit in (1, 2, 3):
            t_parts.append(lax.ppermute(t_mine, 'dp', [(k, k ^ bit) for k in range(4)]))
        dx_cm, sums, z_out, d_w_down = x_post(
            core.astype(jnp.int32).reshape(1), x_gain, x_cm, x_mean, x_rstd, dxn, za_got, zb_got, full, w2_half, w2_got)
        sums, t_sum, acc, d_w_up = finish(
            mesh, sums, t_parts, [*acc_eighths, acc_x, acc_y], [*w1_eighths, w1_x, w1_y])
        d_x_gain, d_x_shift = sums[0, :CH], sums[1, :CH]

        d_m_gain, d_m_shift, d_b_down, d_b_up = (acc[VEC_ROW + k] for k in range(4))
        d_lat, d_z_gain, d_z_shift, d_w_query, d_w_key, d_w_value, d_w_out, d_w_up = final(
            qk_scale, t_sum, acc, latents, row(z_gain), z_norm, queries, w_query, wk_pad, wv_pad, w_out, d_w_up)
        return (z_out, jnp.transpose(dx_cm, (1, 2, 0)), d_lat, d_x_gain, d_x_shift, d_z_gain[0], d_z_shift[0],
                d_w_query, d_w_key, d_w_value, d_w_out, d_m_gain, d_m_shift, d_w_up, d_b_up, d_w_down, d_b_down)

    return jax.shard_map(step, mesh=mesh, in_specs=in_specs, out_specs=out_specs, check_vma=False)
```
